32 devices in a mesh: gx: 4 (over y, x), gy: 2 (over core), gz: 4 (over z).
Axes of the slice: x: 2, y: 2, z: 4, core: 2. Of those that a mesh axis runs over, the one named last changes fastest.
Arguments:
- phi_start: float32 [64, 96, 512], P('gx', 'gy', 'gz'), may hold values from -30 to 30
Outputs:
- phi_final: float32 [64, 96, 512], P('gx', 'gy', 'gz')
- residuals: float32 [3], replicated
The draws below stay inside these ranges and needn't reach their ends.
All inputs are finite; a program needn't handle non-finite values.
Results may differ from the reference program's by a relative error of at most 0.0003.
Values sent between devices are 32-bit elements; how exact they have to be, the bound alone decides.
No kernel may reach another device: no remote copies, remote signals or barrier semaphores. Data moves between devices by JAX's collectives and lax.ppermute only.
A program may use at most 64 MiB of HBM per device.

```python
import math
import jax
import jax.numpy as jnp
from jax import lax

CX = 16
ITERS = 3
NX = 64
NY = 96
NZ = 512


def draw_phi_start(key, part):
    key_phase = jax.random.fold_in(key, 11)
    key_noise = jax.random.fold_in(key, 23)
    phases = jax.random.uniform(key_phase, (3,), jnp.float32, 0.0, 2.0 * math.pi)
    xcoord = jnp.arange(NX, dtype=jnp.float32)[:, None, None] / NX
    ycoord = jnp.arange(NY, dtype=jnp.float32)[None, :, None] / NY
    zcoord = jnp.arange(NZ, dtype=jnp.float32)[None, None, :] / NZ
    smooth = jnp.sin(2.0 * math.pi * 2.0 * xcoord + phases[0])
    smooth = smooth + jnp.sin(2.0 * math.pi * 3.0 * ycoord + phases[1])
    smooth = smooth + jnp.sin(2.0 * math.pi * 2.0 * zcoord + phases[2])
    rough = jnp.clip(0.6 * jax.random.normal(key_noise, (NX, NY, NZ), jnp.float32), -2.4, 2.4)
    scale = jnp.exp(math.log(3.0) * xcoord)
    field = scale * (smooth + rough)
    return field.astype(jnp.float32)


def setup_inputs(seed: int = 0) -> dict:
    key_of = jax.random.split(jax.random.key(seed), 2)
    return {
        "phi_start": draw_phi_start(jax.random.fold_in(key_of[1], 71), 0),
    }


pseudo_step = 0.45

def smooth_sign(field):
    return field / jnp.sqrt(field * field + 1.0)

def upwind_term(back, fwd, positive):
    plus = jnp.maximum(jnp.maximum(back, 0.0) ** 2, jnp.minimum(fwd, 0.0) ** 2)
    minus = jnp.maximum(jnp.minimum(back, 0.0) ** 2, jnp.maximum(fwd, 0.0) ** 2)
    return jnp.where(positive, plus, minus)

def update(ext, sgn):
    center = ext[1:-1, 1:-1, 1:-1]
    positive = sgn > 0.0
    total = upwind_term(center - ext[:-2, 1:-1, 1:-1], ext[2:, 1:-1, 1:-1] - center, positive)
    total = total + upwind_term(center - ext[1:-1, :-2, 1:-1], ext[1:-1, 2:, 1:-1] - center, positive)
    total = total + upwind_term(center - ext[1:-1, 1:-1, :-2], ext[1:-1, 1:-1, 2:] - center, positive)
    return center - pseudo_step * sgn * (jnp.sqrt(total) - 1.0)

def reference(phi_start):
    sgn = smooth_sign(phi_start)
    phi = phi_start
    totals = []
    for step in range(ITERS):
        padded = jnp.pad(phi, 1, mode='edge')

        def slab(index):
            start = (index * CX).astype(jnp.int32)
            ext = lax.dynamic_slice_in_dim(padded, start, CX + 2, 0)
            signs = lax.dynamic_slice_in_dim(sgn, start, CX, 0)
            older = lax.dynamic_slice_in_dim(phi, start, CX, 0)
            newer = update(ext, signs)
            return (newer, jnp.sum((newer - older) * (newer - older)))
        blocks, partial_sums = lax.map(slab, jnp.arange(NX // CX, dtype=jnp.int32))
        totals.append(jnp.sum(partial_sums))
        phi = blocks.reshape(NX, NY, NZ)
    cells = jnp.float32(NX * NY * NZ)
    residuals = jnp.sqrt(jnp.stack(totals) / cells) / pseudo_step
    return (phi, residuals)
```

```python
import functools

import jax
import jax.numpy as jnp
from jax import lax
from jax.experimental import pallas as pl
from jax.experimental.pallas import tpu as pltpu
from jax.sharding import PartitionSpec as P

ITERS = 3
HALO = ITERS
AXES = ("gx", "gy", "gz")
TILE = 8
HALF = 64

pseudo_step = 0.45


def pair_swap(value, partner):
    sizes = [lax.axis_size(a) for a in AXES]

    def flat(place):
        return (place[0] * sizes[1] + place[1]) * sizes[2] + place[2]

    pairs = []
    for i in range(sizes[0]):
        for j in range(sizes[1]):
            for k in range(sizes[2]):
                pairs.append((flat((i, j, k)), flat(partner((i, j, k)))))
    return lax.ppermute(value, AXES, pairs)


def neighbour(dim, colour):
    sizes = [lax.axis_size(a) for a in AXES]

    def partner(place):
        place = list(place)
        here = place[dim]
        there = here ^ 1 if colour == 0 else ((here - 1) ^ 1) + 1
        if 0 <= there < sizes[dim]:
            place[dim] = there
        elif dim != 1 and sizes[1] % 2 == 0:
            place[1] ^= 1
        elif colour == 1 and sizes[dim] % 2 == 0:
            place[dim] = sizes[dim] - 1 - here
        return tuple(place)

    return partner


def exchange(value_even, value_odd, dim):
    first = pair_swap(value_even, neighbour(dim, 0))
    if lax.axis_size(AXES[dim]) == 2:
        return first, first
    return first, pair_swap(value_odd, neighbour(dim, 1))


def sum_over_devices(value):
    sizes = [lax.axis_size(a) for a in AXES]
    if any(n & (n - 1) for n in sizes):
        return lax.psum(value, AXES)
    rounds = []
    for dim in (1, 0, 2):
        bit = 1
        while bit < sizes[dim]:
            rounds.append((dim, bit))
            bit *= 2
    crossed = False
    for dim, bit in rounds:

        def partner(place, dim=dim, bit=bit, flip=crossed):
            place = list(place)
            place[dim] ^= bit
            if flip:
                place[1] ^= 1
            return tuple(place)

        value = value + pair_swap(value, partner)
        crossed = crossed or (dim, bit) == (1, 1)
    return value


def at_ends(axis):
    place = lax.axis_index(axis)
    return place == 0, place == lax.axis_size(axis) - 1


def odd(axis):
    return lax.rem(lax.axis_index(axis), 2) == 1


def low_high(first, second, axis):
    is_odd = odd(axis)
    return jnp.where(is_odd, first, second), jnp.where(is_odd, second, first)


def sign_factors(field):
    sgn = field * lax.rsqrt(field * field + 1.0)
    return jnp.where(field > 0.0, 1.0, -1.0), pseudo_step * sgn


def upwind(sc, s, prev, nxt):
    term = jnp.maximum(sc - jnp.minimum(s * prev, s * nxt), 0.0)
    return term * term


def stepped(c, k, total):
    root = total * lax.rsqrt(jnp.maximum(total, 1e-30))
    return c - k * (root - 1.0)


def plane_pieces(x, sizes, b_ref, xa_ref, xb_ref, ya_ref, yb_ref):
    planes = sizes[0]
    if x < HALO:
        own = low_high(xa_ref[x], xb_ref[x], "gx")[0]
    elif x >= HALO + planes:
        own = low_high(xa_ref[x - HALO - planes], xb_ref[x - HALO - planes], "gx")[1]
    else:
        own = b_ref[x - HALO]
    low, high = low_high(ya_ref[x], yb_ref[x], "gy")
    return own, low, high


def strip_kernel(
    sizes, b_ref, xa_ref, xb_ref, ya_ref, yb_ref, strip_ref, send_ref, lines_ref
):
    planes, rows, lanes = sizes
    wide = planes + 2 * HALO
    pitch = strip_ref.shape[0] // (3 * HALO)
    for x in range(wide):
        own, low, high = plane_pieces(x, sizes, b_ref, xa_ref, xb_ref, ya_ref, yb_ref)
        turned = jnp.concatenate([low, own, high], axis=0).T
        both = jnp.concatenate([turned[0:TILE], turned[lanes - TILE : lanes]], axis=1)
        lines_ref[pl.ds(x, TILE, stride=pitch)] = both
    near = lax.broadcasted_iota(jnp.int32, (pitch, 2 * HALF), 1) < HALF
    shift = TILE - 2 * HALO
    for j in range(3 * HALO):
        low = lines_ref[(j - HALO) * pitch : (j - HALO + 1) * pitch] if j >= HALO else None
        high = lines_ref[(j + shift) * pitch : (j + shift + 1) * pitch] if j < 2 * HALO else None
        if low is None:
            value = high
        elif high is None:
            value = low
        else:
            value = jnp.where(near, low, high)
            send_ref[(j - HALO) * pitch : (j - HALO + 1) * pitch] = value
        strip_ref[j * pitch : (j + 1) * pitch] = value


def main_kernel(
    sizes, b_ref, xa_ref, xb_ref, ya_ref, yb_ref, out_ref, acc_ref, e0, e1, s_ref, k_ref
):
    planes, rows, lanes = sizes
    wide = planes + 2 * HALO
    tall = rows + TILE
    x_first, x_last = at_ends("gx")
    y_first, y_last = at_ends("gy")
    sub = lax.broadcasted_iota(jnp.int32, (TILE, lanes), 0)
    lane = lax.broadcasted_iota(jnp.int32, (TILE, lanes), 1)

    for x in range(wide):
        own, low, high = plane_pieces(x, sizes, b_ref, xa_ref, xb_ref, ya_ref, yb_ref)
        full = jnp.concatenate([own, jnp.where(sub < TILE // 2, high, low)], axis=0)
        e0[x] = full
        s, k = sign_factors(full)
        s_ref[x] = s
        k_ref[x] = k

    def clamp_planes(ref):
        @pl.when(x_first)
        def _():
            ref[HALO - 1] = ref[HALO]

        @pl.when(x_last)
        def _():
            ref[HALO + planes] = ref[HALO + planes - 1]

    def plane_step(src, x):
        c = src[x]
        edge = c[rows:tall]
        edge = jnp.where((sub == TILE - 1) & y_first, c[0:1], edge)
        edge = jnp.where((sub == 0) & y_last, c[rows - 1 : rows], edge)
        around = jnp.concatenate([c[0:rows], edge], axis=0)
        s = s_ref[x]
        sc = s * c
        total = upwind(sc, s, src[x - 1], src[x + 1])
        total = total + upwind(
            sc, s, pltpu.roll(around, 1, 0), pltpu.roll(around, tall - 1, 0)
        )
        total = total + upwind(sc, s, pltpu.roll(c, 1, 1), pltpu.roll(c, lanes - 1, 1))
        new = stepped(c, k_ref[x], total)
        change = new[0:rows] - c[0:rows]
        change = change * change
        part = change[0:TILE]
        for t in range(TILE, rows, TILE):
            part = part + change[t : t + TILE]
        return new, part

    inner = (lane >= HALO) & (lane < lanes - HALO)
    bufs = (e0, e1, e0)
    for it in range(ITERS):
        src = bufs[it]
        clamp_planes(src)
        last = it == ITERS - 1

        def body(x, acc, src=src, it=it, last=last, counted=True):
            new, part = plane_step(src, x)
            if last:
                out_ref[x - HALO] = new[0:rows]
            else:
                bufs[it + 1][x] = new
            return acc + part if counted else acc

        acc = jnp.zeros((TILE, lanes), jnp.float32)
        for x in range(it + 1, HALO):
            body(x, acc, counted=False)
            body(wide - 1 - x, acc, counted=False)
        acc = lax.fori_loop(HALO, HALO + planes, body, acc, unroll=4)
        acc_ref[it] = jnp.where(inner, acc, 0.0)


def edge_kernel(sizes, strip_ref, za_ref, zb_ref, acc_ref, out_ref, sum_ref):
    planes, rows, lanes = sizes
    pitch = strip_ref.shape[0] // (3 * HALO)
    x_first, x_last = at_ends("gx")
    y_first, y_last = at_ends("gy")
    z_first, z_last = at_ends("gz")
    shape = (pitch, 2 * HALF)
    line = lax.broadcasted_iota(jnp.int32, shape, 0)
    lane = lax.broadcasted_iota(jnp.int32, shape, 1)
    near = lane < HALF
    y = jnp.where(near, lane, lane - HALF) - TILE
    x = line - HALO
    low_x = (x == 0) & x_first
    high_x = (x == planes - 1) & x_last
    low_y = (y == 0) & y_first
    high_y = (y == rows - 1) & y_last
    low_z = near & z_first
    high_z = (lane >= HALF) & z_last
    mine = (x >= 0) & (x < planes) & (y >= 0) & (y < rows)

    state = []
    for j in range(3 * HALO):
        own = strip_ref[j * pitch : (j + 1) * pitch]
        if j < HALO:
            got = low_high(
                za_ref[j * pitch : (j + 1) * pitch], zb_ref[j * pitch : (j + 1) * pitch], "gz"
            )[0]
            own = jnp.where(near, pltpu.roll(got, HALF, 1), own)
        elif j >= 2 * HALO:
            i = j - 2 * HALO
            got = low_high(
                za_ref[i * pitch : (i + 1) * pitch], zb_ref[i * pitch : (i + 1) * pitch], "gz"
            )[1]
            own = jnp.where(near, own, pltpu.roll(got, HALF, 1))
        state.append(own)
    factors = [sign_factors(v) for v in state]

    sums = []
    for it in range(ITERS):
        new = list(state)
        change = jnp.zeros(shape, jnp.float32)
        for j in range(it + 1, 3 * HALO - 1 - it):
            c = state[j]
            s, k = factors[j]
            sc = s * c
            total = upwind(
                sc,
                s,
                jnp.where(low_x, c, pltpu.roll(c, 1, 0)),
                jnp.where(high_x, c, pltpu.roll(c, pitch - 1, 0)),
            )
            total = total + upwind(
                sc,
                s,
                jnp.where(low_y, c, pltpu.roll(c, 1, 1)),
                jnp.where(high_y, c, pltpu.roll(c, 2 * HALF - 1, 1)),
            )
            before, after = state[j - 1], state[j + 1]
            if j == HALO:
                before = jnp.where(low_z, c, before)
            if j == 2 * HALO - 1:
                after = jnp.where(high_z, c, after)
            total = total + upwind(sc, s, before, after)
            new[j] = stepped(c, k, total)
            if HALO <= j < 2 * HALO:
                change = change + (new[j] - c) * (new[j] - c)
        state = new
        change = jnp.where(mine, change, 0.0)
        part = acc_ref[it]
        for t in range(0, pitch, TILE):
            part = part + change[t : t + TILE]
        sums.append(jnp.sum(part, axis=0, keepdims=True))
    for i in range(HALO):
        out_ref[i * pitch : (i + 1) * pitch] = state[HALO + i]
    sums.append(jnp.zeros((TILE - ITERS, 2 * HALF), jnp.float32))
    sum_ref[...] = jnp.concatenate(sums, axis=0)


def merge_kernel(sizes, main_ref, edge_ref, out_ref):
    planes, rows, lanes = sizes
    pitch = edge_ref.shape[0] // HALO
    lane = lax.broadcasted_iota(jnp.int32, (rows, lanes), 1)
    for x in range(planes):
        lines = edge_ref[pl.ds(x + HALO, HALO, stride=pitch)]
        lines = jnp.concatenate(
            [lines, jnp.zeros((lanes - HALO, 2 * HALF), jnp.float32)], axis=0
        )
        turned = lines.T
        near = turned[TILE : TILE + rows]
        far = pltpu.roll(turned[HALF + TILE : HALF + TILE + rows], lanes - HALO, 1)
        value = jnp.where(lane < HALO, near, main_ref[x])
        out_ref[x] = jnp.where(lane >= lanes - HALO, far, value)


def vmem(n):
    return [pl.BlockSpec(memory_space=pltpu.VMEM)] * n


def cost(us, nbytes):
    return pl.CostEstimate(flops=int(us * 3.5e6), bytes_accessed=nbytes, transcendentals=0)


def local(phi_start):
    sizes = phi_start.shape
    planes, rows, lanes = sizes
    wide = planes + 2 * HALO
    tall = rows + TILE
    pitch = -(-wide // TILE) * TILE
    f32 = jnp.float32

    low, high = phi_start[:HALO], phi_start[planes - HALO :]
    x_odd, y_odd = odd("gx"), odd("gy")
    xa, xb = exchange(jnp.where(x_odd, low, high), jnp.where(x_odd, high, low), 0)

    tops = jnp.concatenate([t[:, :TILE] for t in (*low_high(xa, xb, "gx"),)], axis=0)
    tails = jnp.concatenate([t[:, rows - TILE :] for t in (*low_high(xa, xb, "gx"),)], axis=0)
    tops = jnp.concatenate([tops[:HALO], phi_start[:, :TILE], tops[HALO:]], axis=0)
    tails = jnp.concatenate([tails[:HALO], phi_start[:, rows - TILE :], tails[HALO:]], axis=0)
    ya, yb = exchange(jnp.where(y_odd, tops, tails), jnp.where(y_odd, tails, tops), 1)

    strip, send = pl.pallas_call(
        functools.partial(strip_kernel, sizes),
        out_shape=(
            jax.ShapeDtypeStruct((3 * HALO * pitch, 2 * HALF), f32),
            jax.ShapeDtypeStruct((HALO * pitch, 2 * HALF), f32),
        ),
        in_specs=vmem(5),
        out_specs=tuple(vmem(2)),
        scratch_shapes=[pltpu.VMEM((TILE * pitch, 2 * HALF), f32)],
        cost_estimate=cost(1, 10**6),
        name="strips",
    )(phi_start, xa, xb, ya, yb)
    za, zb = exchange(send, send, 2)

    inner, acc = pl.pallas_call(
        functools.partial(main_kernel, sizes),
        out_shape=(
            jax.ShapeDtypeStruct(sizes, f32),
            jax.ShapeDtypeStruct((ITERS, TILE, lanes), f32),
        ),
        in_specs=vmem(5),
        out_specs=tuple(vmem(2)),
        scratch_shapes=[pltpu.VMEM((wide, tall, lanes), f32)] * 4,
        cost_estimate=cost(3, 10**6),
        name="inner",
    )(phi_start, xa, xb, ya, yb)

    edge, sums = pl.pallas_call(
        functools.partial(edge_kernel, sizes),
        out_shape=(
            jax.ShapeDtypeStruct((HALO * pitch, 2 * HALF), f32),
            jax.ShapeDtypeStruct((TILE, 2 * HALF), f32),
        ),
        in_specs=vmem(4),
        out_specs=tuple(vmem(2)),
        cost_estimate=cost(1, 10**5),
        name="edges",
    )(strip, za, zb, acc)

    phi_final = pl.pallas_call(
        functools.partial(merge_kernel, sizes),
        out_shape=jax.ShapeDtypeStruct(sizes, f32),
        in_specs=vmem(2),
        out_specs=vmem(1)[0],
        cost_estimate=cost(1, 10**6),
        name="merge",
    )(inner, edge)

    totals = jnp.sum(sum_over_devices(sums)[:ITERS], axis=1)
    cells = planes * rows * lanes
    for axis in AXES:
        cells = cells * lax.axis_size(axis)
    residuals = jnp.sqrt(totals / jnp.float32(cells)) / pseudo_step
    return (phi_final, residuals)


def solution(mesh):
    return jax.shard_map(
        local,
        mesh=mesh,
        in_specs=(P("gx", "gy", "gz"),),
        out_specs=(P("gx", "gy", "gz"), P()),
        check_vma=False,
    )
```

```python
import functools

import jax
import jax.numpy as jnp
from jax import lax
from jax.experimental import pallas as pl
from jax.experimental.pallas import tpu as pltpu
from jax.sharding import PartitionSpec as P

ITERS = 3
HALO = ITERS
AXES = ("gx", "gy", "gz")
TILE = 8
HALF = 64

pseudo_step = 0.45


def pair_swap(value, partner):
    sizes = [lax.axis_size(a) for a in AXES]

    def flat(place):
        return (place[0] * sizes[1] + place[1]) * sizes[2] + place[2]

    pairs = []
    for i in range(sizes[0]):
        for j in range(sizes[1]):
            for k in range(sizes[2]):
                pairs.append((flat((i, j, k)), flat(partner((i, j, k)))))
    return lax.ppermute(value, AXES, pairs)


def neighbour(dim, colour):
    sizes = [lax.axis_size(a) for a in AXES]

    def partner(place):
        place = list(place)
        here = place[dim]
        there = here ^ 1 if colour == 0 else ((here - 1) ^ 1) + 1
        if 0 <= there < sizes[dim]:
            place[dim] = there
        elif dim != 1 and sizes[1] % 2 == 0:
            place[1] ^= 1
        elif colour == 1 and sizes[dim] % 2 == 0:
            place[dim] = sizes[dim] - 1 - here
        return tuple(place)

    return partner


def exchange(value_even, value_odd, dim):
    first = pair_swap(value_even, neighbour(dim, 0))
    if lax.axis_size(AXES[dim]) == 2:
        return first, first
    return first, pair_swap(value_odd, neighbour(dim, 1))


def sum_over_devices(value):
    sizes = [lax.axis_size(a) for a in AXES]
    if any(n & (n - 1) for n in sizes):
        return lax.psum(value, AXES)
    rounds = []
    for dim in (1, 0, 2):
        bit = 1
        while bit < sizes[dim]:
            rounds.append((dim, bit))
            bit *= 2
    crossed = False
    for dim, bit in rounds:

        def partner(place, dim=dim, bit=bit, flip=crossed):
            place = list(place)
            place[dim] ^= bit
            if flip:
                place[1] ^= 1
            return tuple(place)

        value = value + pair_swap(value, partner)
        crossed = crossed or (dim, bit) == (1, 1)
    return value


def at_ends(axis):
    place = lax.axis_index(axis)
    return place == 0, place == lax.axis_size(axis) - 1


def odd(axis):
    return lax.rem(lax.axis_index(axis), 2) == 1


def low_high(first, second, axis):
    is_odd = odd(axis)
    return jnp.where(is_odd, first, second), jnp.where(is_odd, second, first)


def sign_factors(field):
    sgn = field * lax.rsqrt(field * field + 1.0)
    return jnp.where(field > 0.0, 1.0, -1.0), pseudo_step * sgn


def upwind(sc, s, prev, nxt):
    term = jnp.maximum(sc - jnp.minimum(s * prev, s * nxt), 0.0)
    return term * term


def stepped(c, k, total):
    root = total * lax.rsqrt(jnp.maximum(total, 1e-30))
    return c - k * (root - 1.0)


def plane_pieces(x, sizes, b_ref, xa_ref, xb_ref, ya_ref, yb_ref):
    planes = sizes[0]
    if x < HALO:
        own = low_high(xa_ref[x], xb_ref[x], "gx")[0]
    elif x >= HALO + planes:
        own = low_high(xa_ref[x - HALO - planes], xb_ref[x - HALO - planes], "gx")[1]
    else:
        own = b_ref[x - HALO]
    low, high = low_high(ya_ref[x], yb_ref[x], "gy")
    return own, low, high


def strip_kernel(
    sizes, b_ref, xa_ref, xb_ref, ya_ref, yb_ref, strip_ref, send_ref, lines_ref
):
    planes, rows, lanes = sizes
    wide = planes + 2 * HALO
    pitch = strip_ref.shape[0] // (3 * HALO)
    for x in range(wide):
        own, low, high = plane_pieces(x, sizes, b_ref, xa_ref, xb_ref, ya_ref, yb_ref)
        turned = jnp.concatenate([low, own, high], axis=0).T
        both = jnp.concatenate([turned[0:TILE], turned[lanes - TILE : lanes]], axis=1)
        lines_ref[pl.ds(x, TILE, stride=pitch)] = both
    near = lax.broadcasted_iota(jnp.int32, (pitch, 2 * HALF), 1) < HALF
    shift = TILE - 2 * HALO
    for j in range(3 * HALO):
        low = lines_ref[(j - HALO) * pitch : (j - HALO + 1) * pitch] if j >= HALO else None
        high = lines_ref[(j + shift) * pitch : (j + shift + 1) * pitch] if j < 2 * HALO else None
        if low is None:
            value = high
        elif high is None:
            value = low
        else:
            value = jnp.where(near, low, high)
            send_ref[(j - HALO) * pitch : (j - HALO + 1) * pitch] = value
        strip_ref[j * pitch : (j + 1) * pitch] = value


def main_kernel(
    sizes, b_ref, xa_ref, xb_ref, ya_ref, yb_ref, out_ref, acc_ref, e0, e1, s_ref, k_ref
):
    planes, rows, lanes = sizes
    wide = planes + 2 * HALO
    tall = rows + TILE
    x_first, x_last = at_ends("gx")
    y_first, y_last = at_ends("gy")
    sub = lax.broadcasted_iota(jnp.int32, (TILE, lanes), 0)
    lane = lax.broadcasted_iota(jnp.int32, (TILE, lanes), 1)

    for x in range(wide):
        own, low, high = plane_pieces(x, sizes, b_ref, xa_ref, xb_ref, ya_ref, yb_ref)
        full = jnp.concatenate([own, jnp.where(sub < TILE // 2, high, low)], axis=0)
        e0[x] = full
        s, k = sign_factors(full)
        s_ref[x] = s
        k_ref[x] = k

    def clamp_planes(ref):
        @pl.when(x_first)
        def _():
            ref[HALO - 1] = ref[HALO]

        @pl.when(x_last)
        def _():
            ref[HALO + planes] = ref[HALO + planes - 1]

    def plane_step(src, x):
        c = src[x]
        edge = c[rows:tall]
        edge = jnp.where((sub == TILE - 1) & y_first, c[0:1], edge)
        edge = jnp.where((sub == 0) & y_last, c[rows - 1 : rows], edge)
        around = jnp.concatenate([c[0:rows], edge], axis=0)
        s = s_ref[x]
        sc = s * c
        total = upwind(sc, s, src[x - 1], src[x + 1])
        total = total + upwind(
            sc, s, pltpu.roll(around, 1, 0), pltpu.roll(around, tall - 1, 0)
        )
        total = total + upwind(sc, s, pltpu.roll(c, 1, 1), pltpu.roll(c, lanes - 1, 1))
        new = stepped(c, k_ref[x], total)
        change = new[0:rows] - c[0:rows]
        change = change * change
        part = change[0:TILE]
        for t in range(TILE, rows, TILE):
            part = part + change[t : t + TILE]
        return new, part

    inner = (lane >= HALO) & (lane < lanes - HALO)
    bufs = (e0, e1, e0)
    for it in range(ITERS):
        src = bufs[it]
        clamp_planes(src)
        last = it == ITERS - 1

        def body(x, acc, src=src, it=it, last=last, counted=True):
            new, part = plane_step(src, x)
            if last:
                out_ref[x - HALO] = new[0:rows]
            else:
                bufs[it + 1][x] = new
            return acc + part if counted else acc

        acc = jnp.zeros((TILE, lanes), jnp.float32)
        for x in range(it + 1, HALO):
            body(x, acc, counted=False)
            body(wide - 1 - x, acc, counted=False)
        acc = lax.fori_loop(HALO, HALO + planes, body, acc, unroll=4)
        acc_ref[it] = jnp.where(inner, acc, 0.0)


def edge_kernel(sizes, strip_ref, za_ref, zb_ref, acc_ref, out_ref, sum_ref):
    planes, rows, lanes = sizes
    pitch = strip_ref.shape[0] // (3 * HALO)
    x_first, x_last = at_ends("gx")
    y_first, y_last = at_ends("gy")
    z_first, z_last = at_ends("gz")
    shape = (pitch, 2 * HALF)
    line = lax.broadcasted_iota(jnp.int32, shape, 0)
    lane = lax.broadcasted_iota(jnp.int32, shape, 1)
    near = lane < HALF
    y = jnp.where(near, lane, lane - HALF) - TILE
    x = line - HALO
    low_x = (x == 0) & x_first
    high_x = (x == planes - 1) & x_last
    low_y = (y == 0) & y_first
    high_y = (y == rows - 1) & y_last
    low_z = near & z_first
    high_z = (lane >= HALF) & z_last
    mine = (x >= 0) & (x < planes) & (y >= 0) & (y < rows)

    state = []
    for j in range(3 * HALO):
        own = strip_ref[j * pitch : (j + 1) * pitch]
        if j < HALO:
            got = low_high(
                za_ref[j * pitch : (j + 1) * pitch], zb_ref[j * pitch : (j + 1) * pitch], "gz"
            )[0]
            own = jnp.where(near, pltpu.roll(got, HALF, 1), own)
        elif j >= 2 * HALO:
            i = j - 2 * HALO
            got = low_high(
                za_ref[i * pitch : (i + 1) * pitch], zb_ref[i * pitch : (i + 1) * pitch], "gz"
            )[1]
            own = jnp.where(near, own, pltpu.roll(got, HALF, 1))
        state.append(own)
    factors = [sign_factors(v) for v in state]

    sums = []
    for it in range(ITERS):
        new = list(state)
        change = jnp.zeros(shape, jnp.float32)
        for j in range(it + 1, 3 * HALO - 1 - it):
            c = state[j]
            s, k = factors[j]
            sc = s * c
            total = upwind(
                sc,
                s,
                jnp.where(low_x, c, pltpu.roll(c, 1, 0)),
                jnp.where(high_x, c, pltpu.roll(c, pitch - 1, 0)),
            )
            total = total + upwind(
                sc,
                s,
                jnp.where(low_y, c, pltpu.roll(c, 1, 1)),
                jnp.where(high_y, c, pltpu.roll(c, 2 * HALF - 1, 1)),
            )
            before, after = state[j - 1], state[j + 1]
            if j == HALO:
                before = jnp.where(low_z, c, before)
            if j == 2 * HALO - 1:
                after = jnp.where(high_z, c, after)
            total = total + upwind(sc, s, before, after)
            new[j] = stepped(c, k, total)
            if HALO <= j < 2 * HALO:
                change = change + (new[j] - c) * (new[j] - c)
        state = new
        change = jnp.where(mine, change, 0.0)
        part = acc_ref[it]
        for t in range(0, pitch, TILE):
            part = part + change[t : t + TILE]
        sums.append(jnp.sum(part, axis=0, keepdims=True))
    for i in range(HALO):
        out_ref[i * pitch : (i + 1) * pitch] = state[HALO + i]
    sums.append(jnp.zeros((TILE - ITERS, 2 * HALF), jnp.float32))
    sum_ref[...] = jnp.concatenate(sums, axis=0)


def merge_kernel(sizes, main_ref, edge_ref, out_ref):
    planes, rows, lanes = sizes
    pitch = edge_ref.shape[0] // HALO
    lane = lax.broadcasted_iota(jnp.int32, (rows, lanes), 1)
    for x in range(planes):
        lines = edge_ref[pl.ds(x + HALO, HALO, stride=pitch)]
        lines = jnp.concatenate(
            [lines, jnp.zeros((lanes - HALO, 2 * HALF), jnp.float32)], axis=0
        )
        turned = lines.T
        near = turned[TILE : TILE + rows]
        far = pltpu.roll(turned[HALF + TILE : HALF + TILE + rows], lanes - HALO, 1)
        value = jnp.where(lane < HALO, near, main_ref[x])
        out_ref[x] = jnp.where(lane >= lanes - HALO, far, value)


def vmem(n):
    return [pl.BlockSpec(memory_space=pltpu.VMEM)] * n


def grant(mib):
    return pltpu.CompilerParams(vmem_limit_bytes=mib * 2**20)


def cost(us, nbytes):
    return pl.CostEstimate(flops=int(us * 3.5e6), bytes_accessed=nbytes, transcendentals=0)


def local(phi_start):
    sizes = phi_start.shape
    planes, rows, lanes = sizes
    wide = planes + 2 * HALO
    tall = rows + TILE
    pitch = -(-wide // TILE) * TILE
    f32 = jnp.float32

    low, high = phi_start[:HALO], phi_start[planes - HALO :]
    x_odd, y_odd = odd("gx"), odd("gy")
    xa, xb = exchange(jnp.where(x_odd, low, high), jnp.where(x_odd, high, low), 0)

    tops = jnp.concatenate([t[:, :TILE] for t in (*low_high(xa, xb, "gx"),)], axis=0)
    tails = jnp.concatenate([t[:, rows - TILE :] for t in (*low_high(xa, xb, "gx"),)], axis=0)
    tops = jnp.concatenate([tops[:HALO], phi_start[:, :TILE], tops[HALO:]], axis=0)
    tails = jnp.concatenate([tails[:HALO], phi_start[:, rows - TILE :], tails[HALO:]], axis=0)
    ya, yb = exchange(jnp.where(y_odd, tops, tails), jnp.where(y_odd, tails, tops), 1)

    strip, send = pl.pallas_call(
        functools.partial(strip_kernel, sizes),
        out_shape=(
            jax.ShapeDtypeStruct((3 * HALO * pitch, 2 * HALF), f32),
            jax.ShapeDtypeStruct((HALO * pitch, 2 * HALF), f32),
        ),
        in_specs=vmem(5),
        out_specs=tuple(vmem(2)),
        scratch_shapes=[pltpu.VMEM((TILE * pitch, 2 * HALF), f32)],
        cost_estimate=cost(1, 10**6),
        compiler_params=grant(4),
        name="strips",
    )(phi_start, xa, xb, ya, yb)
    za, zb = exchange(send, send, 2)

    inner, acc = pl.pallas_call(
        functools.partial(main_kernel, sizes),
        out_shape=(
            jax.ShapeDtypeStruct(sizes, f32),
            jax.ShapeDtypeStruct((ITERS, TILE, lanes), f32),
        ),
        in_specs=vmem(5),
        out_specs=tuple(vmem(2)),
        scratch_shapes=[pltpu.VMEM((wide, tall, lanes), f32)] * 4,
        cost_estimate=cost(3, 10**6),
        compiler_params=grant(8),
        name="inner",
    )(phi_start, xa, xb, ya, yb)

    edge, sums = pl.pallas_call(
        functools.partial(edge_kernel, sizes),
        out_shape=(
            jax.ShapeDtypeStruct((HALO * pitch, 2 * HALF), f32),
            jax.ShapeDtypeStruct((TILE, 2 * HALF), f32),
        ),
        in_specs=vmem(4),
        out_specs=tuple(vmem(2)),
        cost_estimate=cost(1, 10**5),
        compiler_params=grant(4),
        name="edges",
    )(strip, za, zb, acc)

    phi_final = pl.pallas_call(
        functools.partial(merge_kernel, sizes),
        out_shape=jax.ShapeDtypeStruct(sizes, f32),
        in_specs=vmem(2),
        out_specs=vmem(1)[0],
        cost_estimate=cost(1, 10**6),
        compiler_params=grant(4),
        name="merge",
    )(inner, edge)

    totals = jnp.sum(sum_over_devices(sums)[:ITERS], axis=1)
    cells = planes * rows * lanes
    for axis in AXES:
        cells = cells * lax.axis_size(axis)
    residuals = jnp.sqrt(totals / jnp.float32(cells)) / pseudo_step
    return (phi_final, residuals)


def solution(mesh):
    return jax.shard_map(
        local,
        mesh=mesh,
        in_specs=(P("gx", "gy", "gz"),),
        out_specs=(P("gx", "gy", "gz"), P()),
        check_vma=False,
    )
```

```python
import functools

import jax
import jax.numpy as jnp
from jax import lax
from jax.experimental import pallas as pl
from jax.experimental.pallas import tpu as pltpu
from jax.sharding import PartitionSpec as P

ITERS = 3
HALO = ITERS
AXES = ("gx", "gy", "gz")
TILE = 8
HALF = 64

pseudo_step = 0.45


def pair_swap(value, partner):
    sizes = [lax.axis_size(a) for a in AXES]

    def flat(place):
        return (place[0] * sizes[1] + place[1]) * sizes[2] + place[2]

    pairs = []
    for i in range(sizes[0]):
        for j in range(sizes[1]):
            for k in range(sizes[2]):
                pairs.append((flat((i, j, k)), flat(partner((i, j, k)))))
    return lax.ppermute(value, AXES, pairs)


def neighbour(dim, colour, cross):
    sizes = [lax.axis_size(a) for a in AXES]

    def partner(place):
        place = list(place)
        here = place[dim]
        there = here ^ 1 if colour == 0 else ((here - 1) ^ 1) + 1
        if 0 <= there < sizes[dim]:
            place[dim] = there
            if cross:
                place[1] ^= 1
        elif dim != 1 and sizes[1] % 2 == 0:
            place[1] ^= 1
        elif colour == 1 and sizes[dim] % 2 == 0:
            place[dim] = sizes[dim] - 1 - here
        return tuple(place)

    return partner


def exchange(value_even, value_odd, dim, cross=False):
    first = pair_swap(value_even, neighbour(dim, 0, cross))
    if lax.axis_size(AXES[dim]) == 2:
        return first, first
    return first, pair_swap(value_odd, neighbour(dim, 1, cross))


def other_row(place):
    return (place[0], place[1] ^ 1, place[2])


def sum_over_devices(value):
    sizes = [lax.axis_size(a) for a in AXES]
    if any(n & (n - 1) for n in sizes):
        return lax.psum(value, AXES)
    rounds = []
    for dim in (1, 0, 2):
        bit = 1
        while bit < sizes[dim]:
            rounds.append((dim, bit))
            bit *= 2
    crossed = False
    for dim, bit in rounds:

        def partner(place, dim=dim, bit=bit, flip=crossed):
            place = list(place)
            place[dim] ^= bit
            if flip:
                place[1] ^= 1
            return tuple(place)

        value = value + pair_swap(value, partner)
        crossed = crossed or (dim, bit) == (1, 1)
    return value


def at_ends(axis):
    place = lax.axis_index(axis)
    return place == 0, place == lax.axis_size(axis) - 1


def odd(axis):
    return lax.rem(lax.axis_index(axis), 2) == 1


def low_high(first, second, axis):
    is_odd = odd(axis)
    return jnp.where(is_odd, first, second), jnp.where(is_odd, second, first)


def sign_factors(field):
    sgn = field * lax.rsqrt(field * field + 1.0)
    return jnp.where(field > 0.0, 1.0, -1.0), pseudo_step * sgn


def upwind(sc, s, prev, nxt):
    term = jnp.maximum(sc - jnp.minimum(s * prev, s * nxt), 0.0)
    return term * term


def stepped(c, k, total):
    root = total * lax.rsqrt(jnp.maximum(total, 1e-30))
    return c - k * (root - 1.0)


def faces_kernel(sizes, b_ref, *outs):
    planes, rows, _ = sizes
    x_odd, y_odd = odd("gx"), odd("gy")
    for n, ref in enumerate(outs[:2]):
        low = x_odd if n == 0 else ~x_odd
        ref[...] = b_ref[pl.ds(jnp.where(low, 0, planes - HALO), HALO)]
    for n, ref in enumerate(outs[2:]):
        low = y_odd if n == 0 else ~y_odd
        start = pl.multiple_of(jnp.where(low, 0, rows - TILE), TILE)
        ref[...] = b_ref[:, pl.ds(start, TILE)]


def plane_step(c, s, k, before, after, marks):
    sub, y_first, y_last, rows = marks
    tall, lanes = c.shape
    edge = c[rows:tall]
    edge = jnp.where((sub == TILE - 1) & y_first, c[0:1], edge)
    edge = jnp.where((sub == 0) & y_last, c[rows - 1 : rows], edge)
    around = jnp.concatenate([c[0:rows], edge], axis=0)
    sc = s * c
    total = upwind(sc, s, before, after)
    total = total + upwind(sc, s, pltpu.roll(around, 1, 0), pltpu.roll(around, tall - 1, 0))
    total = total + upwind(sc, s, pltpu.roll(c, 1, 1), pltpu.roll(c, lanes - 1, 1))
    new = stepped(c, k, total)
    change = new[0:rows] - c[0:rows]
    change = change * change
    part = change[0:TILE]
    for t in range(TILE, rows, TILE):
        part = part + change[t : t + TILE]
    return new, part


def plane_marks(sizes):
    _, rows, lanes = sizes
    y_first, y_last = at_ends("gy")
    return lax.broadcasted_iota(jnp.int32, (TILE, lanes), 0), y_first, y_last, rows


def turned_lines(own, mix, lanes):
    turned = jnp.concatenate([mix, own, mix], axis=0).T
    return jnp.concatenate([turned[0:TILE], turned[lanes - TILE : lanes]], axis=1)


def middle(lines_ref, i, pitch, near):
    low = lines_ref[i * pitch : (i + 1) * pitch]
    shift = TILE - HALO
    return jnp.where(near, low, lines_ref[(i + shift) * pitch : (i + shift + 1) * pitch])


def pre_kernel(
    sizes, b_ref, mix_ref, e1_ref, e2_ref, out_ref, s_ref, k_ref, acc_ref, lines_ref, mid_ref, e0
):
    planes, rows, lanes = sizes
    pitch = lines_ref.shape[0] // TILE
    marks = plane_marks(sizes)
    lane = lax.broadcasted_iota(jnp.int32, (TILE, lanes), 1)
    near = lax.broadcasted_iota(jnp.int32, (pitch, 2 * HALF), 1) < HALF

    for p in range(planes):
        own, mix = b_ref[p], mix_ref[p]
        lines_ref[pl.ds(p + HALO, TILE, stride=pitch)] = turned_lines(own, mix, lanes)
        full = jnp.concatenate([own, mix], axis=0)
        e0[p] = full
        s_ref[p], k_ref[p] = sign_factors(full)
    for i in range(HALO):
        mid_ref[i * pitch : (i + 1) * pitch] = middle(lines_ref, i, pitch, near)

    inner = (lane >= HALO) & (lane < lanes - HALO)
    bufs = (e0, e1_ref, e2_ref)
    for it in range(ITERS):

        def body(p, acc, it=it):
            src = bufs[it]
            new, part = plane_step(src[p], s_ref[p], k_ref[p], src[p - 1], src[p + 1], marks)
            if it == ITERS - 1:
                out_ref[p] = new[0:rows]
            else:
                bufs[it + 1][p] = new
            return acc + part

        acc = jnp.zeros((TILE, lanes), jnp.float32)
        acc = lax.fori_loop(it + 1, planes - 1 - it, body, acc, unroll=(7, 6, 5)[it])
        acc_ref[it] = jnp.where(inner, acc, 0.0)


def ends_kernel(sizes, cross, *refs):
    planes, rows, lanes = sizes
    lines_ref, halo_ref, mix_ref = refs[:3]
    if cross:
        mid_ref, held_ref, held_mix_ref = refs[3:6]
    strip_ref, send_ref, lines, given = refs[-4:]
    pitch = lines_ref.shape[0] // TILE
    near = lax.broadcasted_iota(jnp.int32, (pitch, 2 * HALF), 1) < HALF
    lines[...] = lines_ref[...]
    for i in range(2 * HALO):
        x = i if i < HALO else i + planes
        lines[pl.ds(x, TILE, stride=pitch)] = turned_lines(halo_ref[i], mix_ref[i], lanes)
        if cross:
            given[pl.ds(x, TILE, stride=pitch)] = turned_lines(
                held_ref[i], held_mix_ref[i], lanes
            )
    shift = TILE - 2 * HALO
    for j in range(3 * HALO):
        if j < HALO:
            value = lines[(j + shift) * pitch : (j + shift + 1) * pitch]
        elif j >= 2 * HALO:
            value = lines[(j - HALO) * pitch : (j - HALO + 1) * pitch]
        else:
            value = middle(lines, j - HALO, pitch, near)
        strip_ref[j * pitch : (j + 1) * pitch] = value
        i = j - HALO
        if 0 <= i < HALO:
            if cross:
                line = lax.broadcasted_iota(jnp.int32, (pitch, 2 * HALF), 0)
                theirs = (line >= HALO) & (line < HALO + planes)
                value = jnp.where(
                    theirs, mid_ref[i * pitch : (i + 1) * pitch], middle(given, i, pitch, near)
                )
            send_ref[i * pitch : (i + 1) * pitch] = value


def post_kernel(
    sizes,
    b_ref,
    mix_ref,
    halo_ref,
    halo_mix_ref,
    e1_ref,
    e2_ref,
    s_ref,
    k_ref,
    pre_acc_ref,
    out_ref,
    acc_ref,
    f1,
    f2,
):
    planes, rows, lanes = sizes
    x_first, x_last = at_ends("gx")
    marks = plane_marks(sizes)
    lane = lax.broadcasted_iota(jnp.int32, (TILE, lanes), 1)
    inner = (lane >= HALO) & (lane < lanes - HALO)
    factors = {}

    def start(p):
        if 0 <= p < planes:
            return jnp.concatenate([b_ref[p], mix_ref[p]], axis=0)
        i = p + HALO if p < 0 else p - planes + HALO
        return jnp.concatenate([halo_ref[i], halo_mix_ref[i]], axis=0)

    def factor(p):
        if 0 <= p < planes:
            return s_ref[p], k_ref[p]
        if p not in factors:
            factors[p] = sign_factors(start(p))
        return factors[p]

    def get(it, p):
        if it == 0:
            return start(p)
        if it <= p < planes - it:
            return (e1_ref, e2_ref)[it - 1][p]
        return (f1, f2)[it - 1][p + HALO if p < planes // 2 else p - planes + 3 * HALO]

    for it in range(ITERS):
        acc = jnp.zeros((TILE, lanes), jnp.float32)
        lows = range(it + 1 - HALO, it + 1)
        for p in (*lows, *(planes - 1 - p for p in lows)):
            c = get(it, p)
            before, after = get(it, p - 1), get(it, p + 1)
            if p == 0:
                before = jnp.where(x_first, c, before)
            if p == planes - 1:
                after = jnp.where(x_last, c, after)
            s, k = factor(p)
            new, part = plane_step(c, s, k, before, after, marks)
            if it == ITERS - 1:
                out_ref[p if p < HALO else p - planes + 2 * HALO] = new[0:rows]
            else:
                (f1, f2)[it][p + HALO if p < planes // 2 else p - planes + 3 * HALO] = new
            if 0 <= p < planes:
                acc = acc + part
        acc_ref[it] = pre_acc_ref[it] + jnp.where(inner, acc, 0.0)


def edge_kernel(sizes, strip_ref, za_ref, zb_ref, acc_ref, out_ref, sum_ref):
    planes, rows, lanes = sizes
    pitch = strip_ref.shape[0] // (3 * HALO)
    x_first, x_last = at_ends("gx")
    y_first, y_last = at_ends("gy")
    z_first, z_last = at_ends("gz")
    shape = (pitch, 2 * HALF)
    line = lax.broadcasted_iota(jnp.int32, shape, 0)
    lane = lax.broadcasted_iota(jnp.int32, shape, 1)
    near = lane < HALF
    y = jnp.where(near, lane, lane - HALF) - TILE
    x = line - HALO
    low_x = (x == 0) & x_first
    high_x = (x == planes - 1) & x_last
    low_y = (y == 0) & y_first
    high_y = (y == rows - 1) & y_last
    low_z = near & z_first
    high_z = (lane >= HALF) & z_last
    mine = (x >= 0) & (x < planes) & (y >= 0) & (y < rows)

    state = []
    for j in range(3 * HALO):
        own = strip_ref[j * pitch : (j + 1) * pitch]
        if j < HALO:
            got = low_high(
                za_ref[j * pitch : (j + 1) * pitch], zb_ref[j * pitch : (j + 1) * pitch], "gz"
            )[0]
            own = jnp.where(near, pltpu.roll(got, HALF, 1), own)
        elif j >= 2 * HALO:
            i = j - 2 * HALO
            got = low_high(
                za_ref[i * pitch : (i + 1) * pitch], zb_ref[i * pitch : (i + 1) * pitch], "gz"
            )[1]
            own = jnp.where(near, own, pltpu.roll(got, HALF, 1))
        state.append(own)
    factors = [sign_factors(v) for v in state]

    sums = []
    for it in range(ITERS):
        new = list(state)
        change = jnp.zeros(shape, jnp.float32)
        for j in range(it + 1, 3 * HALO - 1 - it):
            c = state[j]
            s, k = factors[j]
            sc = s * c
            total = upwind(
                sc,
                s,
                jnp.where(low_x, c, pltpu.roll(c, 1, 0)),
                jnp.where(high_x, c, pltpu.roll(c, pitch - 1, 0)),
            )
            total = total + upwind(
                sc,
                s,
                jnp.where(low_y, c, pltpu.roll(c, 1, 1)),
                jnp.where(high_y, c, pltpu.roll(c, 2 * HALF - 1, 1)),
            )
            before, after = state[j - 1], state[j + 1]
            if j == HALO:
                before = jnp.where(low_z, c, before)
            if j == 2 * HALO - 1:
                after = jnp.where(high_z, c, after)
            total = total + upwind(sc, s, before, after)
            new[j] = stepped(c, k, total)
            if HALO <= j < 2 * HALO:
                change = change + (new[j] - c) * (new[j] - c)
        state = new
        change = jnp.where(mine, change, 0.0)
        part = acc_ref[it]
        for t in range(0, pitch, TILE):
            part = part + change[t : t + TILE]
        sums.append(jnp.sum(part, axis=0, keepdims=True))
    for i in range(HALO):
        out_ref[i * pitch : (i + 1) * pitch] = state[HALO + i]
    sums.append(jnp.zeros((TILE - ITERS, 2 * HALF), jnp.float32))
    sum_ref[...] = jnp.concatenate(sums, axis=0)


def merge_kernel(sizes, main_ref, ends_ref, edge_ref, out_ref):
    planes, rows, lanes = sizes
    pitch = edge_ref.shape[0] // HALO
    lane = lax.broadcasted_iota(jnp.int32, (rows, lanes), 1)
    for x in range(planes):
        lines = edge_ref[pl.ds(x + HALO, HALO, stride=pitch)]
        lines = jnp.concatenate(
            [lines, jnp.zeros((lanes - HALO, 2 * HALF), jnp.float32)], axis=0
        )
        turned = lines.T
        near = turned[TILE : TILE + rows]
        far = pltpu.roll(turned[HALF + TILE : HALF + TILE + rows], lanes - HALO, 1)
        if x < HALO:
            main = ends_ref[x]
        elif x >= planes - HALO:
            main = ends_ref[x - planes + 2 * HALO]
        else:
            main = main_ref[x]
        value = jnp.where(lane < HALO, near, main)
        out_ref[x] = jnp.where(lane >= lanes - HALO, far, value)


def vmem(n):
    return [pl.BlockSpec(memory_space=pltpu.VMEM)] * n


def grant(mib):
    return pltpu.CompilerParams(vmem_limit_bytes=mib * 2**20)


def cost(us, nbytes):
    return pl.CostEstimate(flops=int(us * 3.5e6), bytes_accessed=nbytes, transcendentals=0)


def call(kernel, sizes, inputs, outputs, scratch, mib, us, name):
    return pl.pallas_call(
        functools.partial(kernel, sizes),
        out_shape=tuple(jax.ShapeDtypeStruct(o, jnp.float32) for o in outputs),
        in_specs=vmem(len(inputs)),
        out_specs=tuple(vmem(len(outputs))),
        scratch_shapes=[pltpu.VMEM(t, jnp.float32) for t in scratch],
        compiler_params=grant(mib),
        cost_estimate=cost(us, 10**6),
        name=name,
    )(*inputs)


def local(phi_start):
    sizes = phi_start.shape
    planes, rows, lanes = sizes
    wide = planes + 2 * HALO
    tall = rows + TILE
    pitch = -(-wide // TILE) * TILE
    cross = lax.axis_size("gy") == 2
    y_odd = odd("gy")

    def mixed(first, second):
        if first is second:
            return first
        low, high = low_high(first, second, "gy")
        sub = lax.broadcasted_iota(jnp.int32, first.shape, 1)
        return jnp.where(sub < TILE // 2, high, low)

    face, tile = (HALO, rows, lanes), (planes, TILE, lanes)
    xs_even, xs_odd, *ys = call(
        faces_kernel,
        sizes,
        (phi_start,),
        (face, face, tile) if cross else (face, face, tile, tile),
        (),
        2,
        0.5,
        "faces",
    )

    xa, xb = exchange(xs_even, xs_odd, 0, cross)
    mix = mixed(*exchange(ys[0], ys[-1], 1))

    block = (planes, tall, lanes)
    e1, e2, inner, s, k, acc, lines, mid = call(
        pre_kernel,
        sizes,
        (phi_start, mix),
        (block, block, sizes, block, block, (ITERS, TILE, lanes))
        + ((TILE * pitch, 2 * HALF), (HALO * pitch, 2 * HALF)),
        (block,),
        8,
        2,
        "pre",
    )

    halo = jnp.concatenate(low_high(xa, xb, "gx"), axis=0)
    first_rows, last_rows = slice(0, TILE), slice(rows - TILE, rows)
    if cross:
        held = halo
        flat = held.reshape(2 * HALO * rows, lanes)
        swapped = pair_swap(jnp.concatenate([flat, mid], axis=0), other_row)
        halo = swapped[: 2 * HALO * rows].reshape(held.shape)
        mid = swapped[2 * HALO * rows :]
        halo_mix = jnp.where(y_odd, held[:, last_rows], held[:, first_rows])
        held_mix = jnp.where(y_odd, halo[:, first_rows], halo[:, last_rows])
        given = (mid, held, held_mix)
    else:
        top, tail = halo[:, first_rows], halo[:, last_rows]
        halo_mix = mixed(
            *exchange(jnp.where(y_odd, top, tail), jnp.where(y_odd, tail, top), 1)
        )
        given = ()

    strip, send = call(
        lambda sizes, *refs: ends_kernel(sizes, cross, *refs),
        sizes,
        (lines, halo, halo_mix, *given),
        ((3 * HALO * pitch, 2 * HALF), (HALO * pitch, 2 * HALF)),
        ((TILE * pitch, 2 * HALF),) * 2,
        4,
        0.5,
        "ends",
    )
    za, zb = exchange(send, send, 2, cross)

    tips, acc = call(
        post_kernel,
        sizes,
        (phi_start, mix, halo, halo_mix, e1, e2, s, k, acc),
        ((2 * HALO, rows, lanes), (ITERS, TILE, lanes)),
        ((4 * HALO, tall, lanes),) * 2,
        8,
        2,
        "post",
    )

    edge, sums = call(
        edge_kernel,
        sizes,
        (strip, za, zb, acc),
        ((HALO * pitch, 2 * HALF), (TILE, 2 * HALF)),
        (),
        4,
        0.5,
        "edges",
    )

    (phi_final,) = call(
        merge_kernel, sizes, (inner, tips, edge), (sizes,), (), 4, 1.5, "merge"
    )

    totals = jnp.sum(sum_over_devices(sums)[:ITERS], axis=1)
    cells = planes * rows * lanes
    for axis in AXES:
        cells = cells * lax.axis_size(axis)
    residuals = jnp.sqrt(totals / jnp.float32(cells)) / pseudo_step
    return (phi_final, residuals)


def solution(mesh):
    return jax.shard_map(
        local,
        mesh=mesh,
        in_specs=(P("gx", "gy", "gz"),),
        out_specs=(P("gx", "gy", "gz"), P()),
        check_vma=False,
    )
```

```python
import functools

import jax
import jax.numpy as jnp
from jax import lax
from jax.experimental import pallas as pl
from jax.experimental.pallas import tpu as pltpu
from jax.sharding import PartitionSpec as P


ITERS = 3
HALO = ITERS
AXES = ("gx", "gy", "gz")
TILE = 8
HALF = 64

pseudo_step = 0.45


def pair_swap(value, partner):
    sizes = [lax.axis_size(a) for a in AXES]

    def flat(place):
        return (place[0] * sizes[1] + place[1]) * sizes[2] + place[2]

    pairs = []
    for i in range(sizes[0]):
        for j in range(sizes[1]):
            for k in range(sizes[2]):
                pairs.append((flat((i, j, k)), flat(partner((i, j, k)))))
    return lax.ppermute(value, AXES, pairs)


def neighbour(dim, colour):
    sizes = [lax.axis_size(a) for a in AXES]

    def partner(place):
        place = list(place)
        here = place[dim]
        there = here ^ 1 if colour == 0 else ((here - 1) ^ 1) + 1
        if 0 <= there < sizes[dim]:
            place[dim] = there
        elif dim != 1 and sizes[1] % 2 == 0:
            place[1] ^= 1
        elif colour == 1 and sizes[dim] % 2 == 0:
            place[dim] = sizes[dim] - 1 - here
        return tuple(place)

    return partner


def exchange(value_even, value_odd, dim):
    first = pair_swap(value_even, neighbour(dim, 0))
    if lax.axis_size(AXES[dim]) == 2:
        return first, first
    return first, pair_swap(value_odd, neighbour(dim, 1))


def sum_over_devices(value):
    sizes = [lax.axis_size(a) for a in AXES]
    if any(n & (n - 1) for n in sizes):
        return lax.psum(value, AXES)
    rounds = []
    for dim in (1, 0, 2):
        bit = 1
        while bit < sizes[dim]:
            rounds.append((dim, bit))
            bit *= 2
    crossed = False
    for dim, bit in rounds:

        def partner(place, dim=dim, bit=bit, flip=crossed):
            place = list(place)
            place[dim] ^= bit
            if flip:
                place[1] ^= 1
            return tuple(place)

        value = value + pair_swap(value, partner)
        crossed = crossed or (dim, bit) == (1, 1)
    return value


def at_ends(axis):
    place = lax.axis_index(axis)
    return place == 0, place == lax.axis_size(axis) - 1


def odd(axis):
    return lax.rem(lax.axis_index(axis), 2) == 1


def low_high(first, second, axis):
    is_odd = odd(axis)
    return jnp.where(is_odd, first, second), jnp.where(is_odd, second, first)


def sign_factors(field):
    sgn = field * lax.rsqrt(field * field + 1.0)
    return jnp.where(field > 0.0, 1.0, -1.0), pseudo_step * sgn


def upwind(sc, s, prev, nxt):
    term = jnp.maximum(sc - jnp.minimum(s * prev, s * nxt), 0.0)
    return term * term


def stepped(c, k, total):
    root = total * lax.rsqrt(jnp.maximum(total, 1e-30))
    return c - k * (root - 1.0)


def tiles_kernel(sizes, b_ref, *outs):
    rows = sizes[1]
    y_odd = odd("gy")
    for n, ref in enumerate(outs):
        low = y_odd if n == 0 else ~y_odd
        start = pl.multiple_of(jnp.where(low, 0, rows - TILE), TILE)
        ref[...] = b_ref[:, pl.ds(start, TILE)]


def plane_step(c, s, k, before, after, marks):
    sub, y_first, y_last, rows = marks
    tall, lanes = c.shape
    edge = c[rows:tall]
    edge = jnp.where((sub == TILE - 1) & y_first, c[0:1], edge)
    edge = jnp.where((sub == 0) & y_last, c[rows - 1 : rows], edge)
    around = jnp.concatenate([c[0:rows], edge], axis=0)
    sc = s * c
    total = upwind(sc, s, before, after)
    total = total + upwind(sc, s, pltpu.roll(around, 1, 0), pltpu.roll(around, tall - 1, 0))
    total = total + upwind(sc, s, pltpu.roll(c, 1, 1), pltpu.roll(c, lanes - 1, 1))
    new = stepped(c, k, total)
    change = new[0:rows] - c[0:rows]
    change = change * change
    part = change[0:TILE]
    for t in range(TILE, rows, TILE):
        part = part + change[t : t + TILE]
    return new, part


def plane_marks(sizes):
    _, rows, lanes = sizes
    y_first, y_last = at_ends("gy")
    return lax.broadcasted_iota(jnp.int32, (TILE, lanes), 0), y_first, y_last, rows


def turned_lines(own, mix, lanes):
    turned = jnp.concatenate([mix, own, mix], axis=0).T
    return jnp.concatenate([turned[0:TILE], turned[lanes - TILE : lanes]], axis=1)


def middle(lines_ref, i, pitch, near):
    low = lines_ref[i * pitch : (i + 1) * pitch]
    shift = TILE - HALO
    return jnp.where(near, low, lines_ref[(i + shift) * pitch : (i + shift + 1) * pitch])


def fronts_kernel(sizes, b_ref, mix_ref, la_ref, lb_ref, xa_ref, xb_ref):
    planes, rows, lanes = sizes
    x_odd = odd("gx")
    low = [turned_lines(b_ref[p], mix_ref[p], lanes) for p in range(HALO)]
    high = [turned_lines(b_ref[p], mix_ref[p], lanes) for p in range(planes - HALO, planes)]
    for i in range(HALO):
        here = pl.ds(i * TILE, TILE)
        la_ref[here] = jnp.where(x_odd, low[i], high[i])
        lb_ref[here] = jnp.where(x_odd, high[i], low[i])
    for ref, is_low in ((xa_ref, x_odd), (xb_ref, ~x_odd)):
        start = jnp.where(is_low, 0, planes - HALO)
        ref[:, 0:rows] = b_ref[pl.ds(start, HALO)]
        ref[:, rows : rows + TILE] = mix_ref[pl.ds(start, HALO)]


def lines_kernel(sizes, b_ref, mix_ref, lines_ref):
    planes, _, lanes = sizes
    pitch = lines_ref.shape[0] // TILE
    for p in range(planes):
        lines_ref[pl.ds(p + HALO, TILE, stride=pitch)] = turned_lines(
            b_ref[p], mix_ref[p], lanes
        )


def pre_kernel(sizes, b_ref, mix_ref, e1_ref, e2_ref, out_ref, s_ref, k_ref, acc_ref, e0):
    planes, rows, lanes = sizes
    marks = plane_marks(sizes)
    lane = lax.broadcasted_iota(jnp.int32, (TILE, lanes), 1)

    for p in range(planes):
        full = jnp.concatenate([b_ref[p], mix_ref[p]], axis=0)
        e0[p] = full
        s_ref[p], k_ref[p] = sign_factors(full)

    inner = (lane >= HALO) & (lane < lanes - HALO)
    bufs = (e0, e1_ref, e2_ref)
    for it in range(ITERS):

        def body(p, acc, it=it):
            src = bufs[it]
            new, part = plane_step(src[p], s_ref[p], k_ref[p], src[p - 1], src[p + 1], marks)
            if it == ITERS - 1:
                out_ref[p] = new[0:rows]
            else:
                bufs[it + 1][p] = new
            return acc + part

        acc = jnp.zeros((TILE, lanes), jnp.float32)
        acc = lax.fori_loop(it + 1, planes - 1 - it, body, acc, unroll=(7, 6, 5)[it])
        acc_ref[it] = jnp.where(inner, acc, 0.0)


def ends_kernel(sizes, lines_ref, la_ref, lb_ref, strip_ref, send_ref, lines):
    planes = sizes[0]
    pitch = lines_ref.shape[0] // TILE
    near = lax.broadcasted_iota(jnp.int32, (pitch, 2 * HALF), 1) < HALF
    lines[...] = lines_ref[...]
    low, high = low_high(la_ref[...], lb_ref[...], "gx")
    for i in range(HALO):
        here = slice(i * TILE, (i + 1) * TILE)
        lines[pl.ds(i, TILE, stride=pitch)] = low[here]
        lines[pl.ds(i + HALO + planes, TILE, stride=pitch)] = high[here]
    shift = TILE - 2 * HALO
    for j in range(3 * HALO):
        if j < HALO:
            value = lines[(j + shift) * pitch : (j + shift + 1) * pitch]
        elif j >= 2 * HALO:
            value = lines[(j - HALO) * pitch : (j - HALO + 1) * pitch]
        else:
            value = middle(lines, j - HALO, pitch, near)
            send_ref[(j - HALO) * pitch : (j - HALO + 1) * pitch] = value
        strip_ref[j * pitch : (j + 1) * pitch] = value


def post_kernel(
    sizes,
    b_ref,
    mix_ref,
    xa_ref,
    xb_ref,
    e1_ref,
    e2_ref,
    s_ref,
    k_ref,
    pre_acc_ref,
    out_ref,
    acc_ref,
    f1,
    f2,
):
    planes, rows, lanes = sizes
    x_first, x_last = at_ends("gx")
    marks = plane_marks(sizes)
    lane = lax.broadcasted_iota(jnp.int32, (TILE, lanes), 1)
    inner = (lane >= HALO) & (lane < lanes - HALO)
    factors = {}

    def start(p):
        if 0 <= p < planes:
            return jnp.concatenate([b_ref[p], mix_ref[p]], axis=0)
        i = p + HALO if p < 0 else p - planes
        return low_high(xa_ref[i], xb_ref[i], "gx")[0 if p < 0 else 1]

    def factor(p):
        if 0 <= p < planes:
            return s_ref[p], k_ref[p]
        if p not in factors:
            factors[p] = sign_factors(start(p))
        return factors[p]

    def get(it, p):
        if it == 0:
            return start(p)
        if it <= p < planes - it:
            return (e1_ref, e2_ref)[it - 1][p]
        return (f1, f2)[it - 1][p + HALO if p < planes // 2 else p - planes + 3 * HALO]

    for it in range(ITERS):
        acc = jnp.zeros((TILE, lanes), jnp.float32)
        lows = range(it + 1 - HALO, it + 1)
        for p in (*lows, *(planes - 1 - p for p in lows)):
            c = get(it, p)
            before, after = get(it, p - 1), get(it, p + 1)
            if p == 0:
                before = jnp.where(x_first, c, before)
            if p == planes - 1:
                after = jnp.where(x_last, c, after)
            s, k = factor(p)
            new, part = plane_step(c, s, k, before, after, marks)
            if it == ITERS - 1:
                out_ref[p if p < HALO else p - planes + 2 * HALO] = new[0:rows]
            else:
                (f1, f2)[it][p + HALO if p < planes // 2 else p - planes + 3 * HALO] = new
            if 0 <= p < planes:
                acc = acc + part
        acc_ref[it] = pre_acc_ref[it] + jnp.where(inner, acc, 0.0)


def edge_kernel(sizes, strip_ref, za_ref, zb_ref, acc_ref, out_ref, sum_ref):
    planes, rows, _ = sizes
    pitch = strip_ref.shape[0] // (3 * HALO)
    x_first, x_last = at_ends("gx")
    y_first, y_last = at_ends("gy")
    z_first, z_last = at_ends("gz")
    shape = (pitch, 2 * HALF)
    line = lax.broadcasted_iota(jnp.int32, shape, 0)
    lane = lax.broadcasted_iota(jnp.int32, shape, 1)
    near = lane < HALF
    y = jnp.where(near, lane, lane - HALF) - TILE
    x = line - HALO
    low_x = (x == 0) & x_first
    high_x = (x == planes - 1) & x_last
    low_y = (y == 0) & y_first
    high_y = (y == rows - 1) & y_last
    low_z = near & z_first
    high_z = (lane >= HALF) & z_last
    mine = (x >= 0) & (x < planes) & (y >= 0) & (y < rows)

    state = []
    for j in range(3 * HALO):
        own = strip_ref[j * pitch : (j + 1) * pitch]
        if j < HALO:
            got = low_high(
                za_ref[j * pitch : (j + 1) * pitch], zb_ref[j * pitch : (j + 1) * pitch], "gz"
            )[0]
            own = jnp.where(near, pltpu.roll(got, HALF, 1), own)
        elif j >= 2 * HALO:
            i = j - 2 * HALO
            got = low_high(
                za_ref[i * pitch : (i + 1) * pitch], zb_ref[i * pitch : (i + 1) * pitch], "gz"
            )[1]
            own = jnp.where(near, own, pltpu.roll(got, HALF, 1))
        state.append(own)
    factors = [sign_factors(v) for v in state]

    sums = []
    for it in range(ITERS):
        new = list(state)
        change = jnp.zeros(shape, jnp.float32)
        for j in range(it + 1, 3 * HALO - 1 - it):
            c = state[j]
            s, k = factors[j]
            sc = s * c
            total = upwind(
                sc,
                s,
                jnp.where(low_x, c, pltpu.roll(c, 1, 0)),
                jnp.where(high_x, c, pltpu.roll(c, pitch - 1, 0)),
            )
            total = total + upwind(
                sc,
                s,
                jnp.where(low_y, c, pltpu.roll(c, 1, 1)),
                jnp.where(high_y, c, pltpu.roll(c, 2 * HALF - 1, 1)),
            )
            before, after = state[j - 1], state[j + 1]
            if j == HALO:
                before = jnp.where(low_z, c, before)
            if j == 2 * HALO - 1:
                after = jnp.where(high_z, c, after)
            total = total + upwind(sc, s, before, after)
            new[j] = stepped(c, k, total)
            if HALO <= j < 2 * HALO:
                change = change + (new[j] - c) * (new[j] - c)
        state = new
        change = jnp.where(mine, change, 0.0)
        part = acc_ref[it]
        for t in range(0, pitch, TILE):
            part = part + change[t : t + TILE]
        sums.append(jnp.sum(part, axis=0, keepdims=True))
    for i in range(HALO):
        out_ref[i * pitch : (i + 1) * pitch] = state[HALO + i]
    sums.append(jnp.zeros((TILE - ITERS, 2 * HALF), jnp.float32))
    sum_ref[...] = jnp.concatenate(sums, axis=0)


def merge_kernel(sizes, main_ref, ends_ref, edge_ref, out_ref):
    planes, rows, lanes = sizes
    pitch = edge_ref.shape[0] // HALO
    lane = lax.broadcasted_iota(jnp.int32, (rows, lanes), 1)
    for x in range(planes):
        lines = edge_ref[pl.ds(x + HALO, HALO, stride=pitch)]
        lines = jnp.concatenate(
            [lines, jnp.zeros((lanes - HALO, 2 * HALF), jnp.float32)], axis=0
        )
        turned = lines.T
        near = turned[TILE : TILE + rows]
        far = pltpu.roll(turned[HALF + TILE : HALF + TILE + rows], lanes - HALO, 1)
        if x < HALO:
            main = ends_ref[x]
        elif x >= planes - HALO:
            main = ends_ref[x - planes + 2 * HALO]
        else:
            main = main_ref[x]
        value = jnp.where(lane < HALO, near, main)
        out_ref[x] = jnp.where(lane >= lanes - HALO, far, value)


def vmem(n):
    return [pl.BlockSpec(memory_space=pltpu.VMEM)] * n


def grant(mib):
    return pltpu.CompilerParams(vmem_limit_bytes=mib * 2**20)


def cost(us, nbytes):
    return pl.CostEstimate(flops=int(us * 3.5e6), bytes_accessed=nbytes, transcendentals=0)


def call(kernel, sizes, inputs, outputs, scratch, mib, us):
    return pl.pallas_call(
        functools.partial(kernel, sizes),
        out_shape=tuple(jax.ShapeDtypeStruct(o, jnp.float32) for o in outputs),
        in_specs=vmem(len(inputs)),
        out_specs=tuple(vmem(len(outputs))),
        scratch_shapes=[pltpu.VMEM(t, jnp.float32) for t in scratch],
        compiler_params=grant(mib),
        cost_estimate=cost(us, 10**6),
    )(*inputs)


def local(phi_start):
    sizes = phi_start.shape
    planes, rows, lanes = sizes
    wide = planes + 2 * HALO
    tall = rows + TILE
    pitch = -(-wide // TILE) * TILE

    def mixed(first, second):
        if first is second:
            return first
        low, high = low_high(first, second, "gy")
        sub = lax.broadcasted_iota(jnp.int32, first.shape, 1)
        return jnp.where(sub < TILE // 2, high, low)

    colours = 1 if lax.axis_size("gy") == 2 else 2
    ys = call(tiles_kernel, sizes, (phi_start,), ((planes, TILE, lanes),) * colours, (), 2, 0.2)
    mix = mixed(*exchange(ys[0], ys[-1], 1))

    line, front = (HALO * TILE, 2 * HALF), (HALO, tall, lanes)
    la, lb, xa, xb = call(
        fronts_kernel, sizes, (phi_start, mix), (line, line, front, front), (), 2, 0.2
    )
    la, lb = exchange(la, lb, 0)
    xa, xb = exchange(xa, xb, 0)

    (lines,) = call(lines_kernel, sizes, (phi_start, mix), ((TILE * pitch, 2 * HALF),), (), 2, 0.5)
    strip, send = call(
        ends_kernel,
        sizes,
        (lines, la, lb),
        ((3 * HALO * pitch, 2 * HALF), (HALO * pitch, 2 * HALF)),
        ((TILE * pitch, 2 * HALF),),
        4,
        0.2,
    )
    za, zb = exchange(send, send, 2)

    block = (planes, tall, lanes)
    e1, e2, inner, s, k, acc = call(
        pre_kernel,
        sizes,
        (phi_start, mix),
        (block, block, sizes, block, block, (ITERS, TILE, lanes)),
        (block,),
        8,
        1.5,
    )
    tips, acc = call(
        post_kernel,
        sizes,
        (phi_start, mix, xa, xb, e1, e2, s, k, acc),
        ((2 * HALO, rows, lanes), (ITERS, TILE, lanes)),
        ((4 * HALO, tall, lanes),) * 2,
        8,
        0.6,
    )

    edge, sums = call(
        edge_kernel,
        sizes,
        (strip, za, zb, acc),
        ((HALO * pitch, 2 * HALF), (TILE, 2 * HALF)),
        (),
        4,
        0.5,
    )

    (phi_final,) = call(merge_kernel, sizes, (inner, tips, edge), (sizes,), (), 4, 1.5)

    totals = jnp.sum(sum_over_devices(sums)[:ITERS], axis=1)
    cells = planes * rows * lanes
    for axis in AXES:
        cells = cells * lax.axis_size(axis)
    residuals = jnp.sqrt(totals / jnp.float32(cells)) / pseudo_step
    return (phi_final, residuals)


def solution(mesh):
    return jax.shard_map(
        local,
        mesh=mesh,
        in_specs=(P("gx", "gy", "gz"),),
        out_specs=(P("gx", "gy", "gz"), P()),
        check_vma=False,
    )
```

```python
import functools

import jax
import jax.numpy as jnp
from jax import lax
from jax.experimental import pallas as pl
from jax.experimental.pallas import tpu as pltpu
from jax.sharding import PartitionSpec as P


ITERS = 3
HALO = ITERS
AXES = ("gx", "gy", "gz")
TILE = 8
HALF = 64

pseudo_step = 0.45


def pair_swap(value, partner):
    sizes = [lax.axis_size(a) for a in AXES]

    def flat(place):
        return (place[0] * sizes[1] + place[1]) * sizes[2] + place[2]

    pairs = []
    for i in range(sizes[0]):
        for j in range(sizes[1]):
            for k in range(sizes[2]):
                pairs.append((flat((i, j, k)), flat(partner((i, j, k)))))
    return lax.ppermute(value, AXES, pairs)


def neighbour(dim, colour, cross):
    sizes = [lax.axis_size(a) for a in AXES]

    def partner(place):
        place = list(place)
        here = place[dim]
        there = here ^ 1 if colour == 0 else ((here - 1) ^ 1) + 1
        if 0 <= there < sizes[dim]:
            place[dim] = there
            if cross:
                place[1] ^= 1
        elif dim != 1 and sizes[1] % 2 == 0:
            place[1] ^= 1
        elif colour == 1 and sizes[dim] % 2 == 0:
            place[dim] = sizes[dim] - 1 - here
        return tuple(place)

    return partner


def exchange(value_even, value_odd, dim, cross=False):
    first = pair_swap(value_even, neighbour(dim, 0, cross))
    if lax.axis_size(AXES[dim]) == 2:
        return first, first
    return first, pair_swap(value_odd, neighbour(dim, 1, cross))


def sum_over_devices(value):
    sizes = [lax.axis_size(a) for a in AXES]
    if any(n & (n - 1) for n in sizes):
        return lax.psum(value, AXES)
    rounds = []
    for dim in (1, 0, 2):
        bit = 1
        while bit < sizes[dim]:
            rounds.append((dim, bit))
            bit *= 2
    crossed = False
    for dim, bit in rounds:

        def partner(place, dim=dim, bit=bit, flip=crossed):
            place = list(place)
            place[dim] ^= bit
            if flip:
                place[1] ^= 1
            return tuple(place)

        value = value + pair_swap(value, partner)
        crossed = crossed or (dim, bit) == (1, 1)
    return value


def at_ends(axis):
    place = lax.axis_index(axis)
    return place == 0, place == lax.axis_size(axis) - 1


def odd(axis):
    return lax.rem(lax.axis_index(axis), 2) == 1


def low_high(first, second, axis):
    is_odd = odd(axis)
    return jnp.where(is_odd, first, second), jnp.where(is_odd, second, first)


def sign_factors(field):
    sgn = field * lax.rsqrt(field * field + 1.0)
    return jnp.where(field > 0.0, 1.0, -1.0), pseudo_step * sgn


def upwind(sc, s, prev, nxt):
    term = jnp.maximum(sc - jnp.minimum(s * prev, s * nxt), 0.0)
    return term * term


def stepped(c, k, total):
    root = total * lax.rsqrt(jnp.maximum(total, 1e-30))
    return c - k * (root - 1.0)


def tiles_kernel(sizes, b_ref, *outs):
    rows = sizes[1]
    y_odd = odd("gy")
    for n, ref in enumerate(outs):
        low = y_odd if n == 0 else ~y_odd
        start = pl.multiple_of(jnp.where(low, 0, rows - TILE), TILE)
        ref[...] = b_ref[:, pl.ds(start, TILE)]


def plane_step(c, s, k, before, after, marks):
    sub, y_first, y_last, rows = marks
    tall, lanes = c.shape
    edge = c[rows:tall]
    edge = jnp.where((sub == TILE - 1) & y_first, c[0:1], edge)
    edge = jnp.where((sub == 0) & y_last, c[rows - 1 : rows], edge)
    around = jnp.concatenate([c[0:rows], edge], axis=0)
    sc = s * c
    total = upwind(sc, s, before, after)
    total = total + upwind(sc, s, pltpu.roll(around, 1, 0), pltpu.roll(around, tall - 1, 0))
    total = total + upwind(sc, s, pltpu.roll(c, 1, 1), pltpu.roll(c, lanes - 1, 1))
    new = stepped(c, k, total)
    change = new[0:rows] - c[0:rows]
    change = change * change
    part = change[0:TILE]
    for t in range(TILE, rows, TILE):
        part = part + change[t : t + TILE]
    return new, part


def plane_marks(sizes):
    _, rows, lanes = sizes
    y_first, y_last = at_ends("gy")
    return lax.broadcasted_iota(jnp.int32, (TILE, lanes), 0), y_first, y_last, rows


def turned_lines(own, mix, lanes):
    turned = jnp.concatenate([mix, own, mix], axis=0).T
    return jnp.concatenate([turned[0:TILE], turned[lanes - TILE : lanes]], axis=1)


def middle(lines_ref, i, pitch, near):
    low = lines_ref[i * pitch : (i + 1) * pitch]
    shift = TILE - HALO
    return jnp.where(near, low, lines_ref[(i + shift) * pitch : (i + shift + 1) * pitch])


def pair_tiles_kernel(sizes, b_ref, out_ref):
    planes, rows, lanes = sizes
    start = pl.multiple_of(jnp.where(odd("gy"), 0, rows - TILE), TILE)
    for p in range(planes):
        plane = b_ref[p]
        out_ref[p * TILE : (p + 1) * TILE] = b_ref[p, pl.ds(start, TILE)]
        out_ref[(planes + p) * TILE : (planes + p + 1) * TILE] = turned_lines(
            plane, plane[0:TILE], lanes
        )


def pair_lines(sizes, mine_ref, theirs_ref):
    planes, rows, _ = sizes
    lane = lax.rem(lax.broadcasted_iota(jnp.int32, (TILE, 2 * HALF), 1), HALF)
    inside = (lane >= TILE) & (lane < TILE + rows)
    y_odd = odd("gy")
    up, down = rows, 2 * HALF - rows

    def lines(p):
        here = slice((planes + p) * TILE, (planes + p + 1) * TILE)
        mine, theirs = mine_ref[here], theirs_ref[here]
        beside_mine = pltpu.roll(theirs, jnp.where(y_odd, down, up), 1)
        beside_theirs = pltpu.roll(mine, jnp.where(y_odd, up, down), 1)
        return jnp.where(inside, mine, beside_mine), jnp.where(inside, theirs, beside_theirs)

    return lines


def own_lines(sizes, b_ref, mix_ref):
    return lambda p: (turned_lines(b_ref[p], mix_ref[p], sizes[2]),)


def fronts_kernel(sizes, paired, b_ref, mix_ref, *refs):
    planes, rows, _ = sizes
    la_ref, lb_ref, xa_ref, xb_ref = refs[-4:]
    lines = pair_lines(sizes, *refs[:2]) if paired else own_lines(sizes, b_ref, mix_ref)
    x_odd = odd("gx")
    for i in range(HALO):
        for n, (low, high) in enumerate(zip(lines(i), lines(planes - HALO + i))):
            here = pl.ds((n * HALO + i) * TILE, TILE)
            la_ref[here] = jnp.where(x_odd, low, high)
            lb_ref[here] = jnp.where(x_odd, high, low)
    for ref, is_low in ((xa_ref, x_odd), (xb_ref, ~x_odd)):
        start = jnp.where(is_low, 0, planes - HALO)
        ref[:, 0:rows] = b_ref[pl.ds(start, HALO)]
        ref[:, rows : rows + TILE] = mix_ref[pl.ds(start, HALO)]


def lines_kernel(sizes, paired, first_ref, second_ref, *outs):
    planes = sizes[0]
    pitch = outs[0].shape[0] // TILE
    lines = (pair_lines if paired else own_lines)(sizes, first_ref, second_ref)
    for p in range(planes):
        for ref, value in zip(outs, lines(p)):
            ref[pl.ds(p + HALO, TILE, stride=pitch)] = value


def pre_kernel(sizes, b_ref, mix_ref, e1_ref, e2_ref, out_ref, s_ref, k_ref, acc_ref, e0):
    planes, rows, lanes = sizes
    marks = plane_marks(sizes)
    lane = lax.broadcasted_iota(jnp.int32, (TILE, lanes), 1)

    for p in range(planes):
        full = jnp.concatenate([b_ref[p], mix_ref[p]], axis=0)
        e0[p] = full
        s_ref[p], k_ref[p] = sign_factors(full)

    inner = (lane >= HALO) & (lane < lanes - HALO)
    bufs = (e0, e1_ref, e2_ref)
    for it in range(ITERS):

        def body(p, acc, it=it):
            src = bufs[it]
            new, part = plane_step(src[p], s_ref[p], k_ref[p], src[p - 1], src[p + 1], marks)
            if it == ITERS - 1:
                out_ref[p] = new[0:rows]
            else:
                bufs[it + 1][p] = new
            return acc + part

        acc = jnp.zeros((TILE, lanes), jnp.float32)
        acc = lax.fori_loop(it + 1, planes - 1 - it, body, acc, unroll=(7, 6, 5)[it])
        acc_ref[it] = jnp.where(inner, acc, 0.0)


def ends_kernel(sizes, paired, *refs):
    planes = sizes[0]
    kinds = 2 if paired else 1
    la_ref, lb_ref, strip_ref, sa_ref, sb_ref = refs[kinds : kinds + 5]
    sets = refs[kinds + 5 :]
    pitch = refs[0].shape[0] // TILE
    near = lax.broadcasted_iota(jnp.int32, (pitch, 2 * HALF), 1) < HALF
    low, high = low_high(la_ref[...], lb_ref[...], "gx")
    for n in range(kinds):
        lines = sets[n]
        lines[...] = refs[n][...]
        for i in range(HALO):
            k = (kinds - 1 - n) * HALO + i
            here = slice(k * TILE, (k + 1) * TILE)
            lines[pl.ds(i, TILE, stride=pitch)] = low[here]
            lines[pl.ds(i + HALO + planes, TILE, stride=pitch)] = high[here]
    lines, given = sets[0], sets[kinds - 1]
    shift = TILE - 2 * HALO
    for j in range(3 * HALO):
        if j < HALO:
            value = lines[(j + shift) * pitch : (j + shift + 1) * pitch]
        elif j >= 2 * HALO:
            value = lines[(j - HALO) * pitch : (j - HALO + 1) * pitch]
        else:
            value = middle(lines, j - HALO, pitch, near)
        strip_ref[j * pitch : (j + 1) * pitch] = value
    layers = [middle(given, i, pitch, near) for i in range(HALO)]
    swung = [pltpu.roll(v, HALF, 1) for v in layers]
    z_odd = odd("gz")
    for i in range(0, HALO, 2):
        if i + 1 < HALO:
            to_low = jnp.where(near, layers[i], swung[i + 1])
            to_high = jnp.where(near, swung[i], layers[i + 1])
        else:
            to_low, to_high = layers[i], swung[i]
        here = slice(i // 2 * pitch, (i // 2 + 1) * pitch)
        sa_ref[here] = jnp.where(z_odd, to_low, to_high)
        sb_ref[here] = jnp.where(z_odd, to_high, to_low)


def post_kernel(
    sizes,
    b_ref,
    mix_ref,
    xa_ref,
    xb_ref,
    e1_ref,
    e2_ref,
    s_ref,
    k_ref,
    pre_acc_ref,
    out_ref,
    acc_ref,
    f1,
    f2,
):
    planes, rows, lanes = sizes
    x_first, x_last = at_ends("gx")
    marks = plane_marks(sizes)
    lane = lax.broadcasted_iota(jnp.int32, (TILE, lanes), 1)
    inner = (lane >= HALO) & (lane < lanes - HALO)
    factors = {}

    def start(p):
        if 0 <= p < planes:
            return jnp.concatenate([b_ref[p], mix_ref[p]], axis=0)
        i = p + HALO if p < 0 else p - planes
        return low_high(xa_ref[i], xb_ref[i], "gx")[0 if p < 0 else 1]

    def factor(p):
        if 0 <= p < planes:
            return s_ref[p], k_ref[p]
        if p not in factors:
            factors[p] = sign_factors(start(p))
        return factors[p]

    def get(it, p):
        if it == 0:
            return start(p)
        if it <= p < planes - it:
            return (e1_ref, e2_ref)[it - 1][p]
        return (f1, f2)[it - 1][p + HALO if p < planes // 2 else p - planes + 3 * HALO]

    for it in range(ITERS):
        acc = jnp.zeros((TILE, lanes), jnp.float32)
        lows = range(it + 1 - HALO, it + 1)
        for p in (*lows, *(planes - 1 - p for p in lows)):
            c = get(it, p)
            before, after = get(it, p - 1), get(it, p + 1)
            if p == 0:
                before = jnp.where(x_first, c, before)
            if p == planes - 1:
                after = jnp.where(x_last, c, after)
            s, k = factor(p)
            new, part = plane_step(c, s, k, before, after, marks)
            if it == ITERS - 1:
                out_ref[p if p < HALO else p - planes + 2 * HALO] = new[0:rows]
            else:
                (f1, f2)[it][p + HALO if p < planes // 2 else p - planes + 3 * HALO] = new
            if 0 <= p < planes:
                acc = acc + part
        acc_ref[it] = pre_acc_ref[it] + jnp.where(inner, acc, 0.0)


def edge_kernel(sizes, strip_ref, za_ref, zb_ref, acc_ref, out_ref, sum_ref):
    planes, rows, _ = sizes
    pitch = strip_ref.shape[0] // (3 * HALO)
    x_first, x_last = at_ends("gx")
    y_first, y_last = at_ends("gy")
    z_first, z_last = at_ends("gz")
    shape = (pitch, 2 * HALF)
    line = lax.broadcasted_iota(jnp.int32, shape, 0)
    lane = lax.broadcasted_iota(jnp.int32, shape, 1)
    near = lane < HALF
    y = jnp.where(near, lane, lane - HALF) - TILE
    x = line - HALO
    low_x = (x == 0) & x_first
    high_x = (x == planes - 1) & x_last
    low_y = (y == 0) & y_first
    high_y = (y == rows - 1) & y_last
    low_z = near & z_first
    high_z = (lane >= HALF) & z_last
    mine = (x >= 0) & (x < planes) & (y >= 0) & (y < rows)

    state = []
    packs = [
        low_high(za_ref[n : n + pitch], zb_ref[n : n + pitch], "gz")
        for n in range(0, za_ref.shape[0], pitch)
    ]
    for j in range(3 * HALO):
        own = strip_ref[j * pitch : (j + 1) * pitch]
        if j < HALO:
            got = packs[j // 2][0]
            got = got if j % 2 == 0 else pltpu.roll(got, HALF, 1)
            own = jnp.where(near, got, own)
        elif j >= 2 * HALO:
            i = j - 2 * HALO
            got = packs[i // 2][1]
            got = pltpu.roll(got, HALF, 1) if i % 2 == 0 else got
            own = jnp.where(near, own, got)
        state.append(own)
    factors = [sign_factors(v) for v in state]

    sums = []
    for it in range(ITERS):
        new = list(state)
        change = jnp.zeros(shape, jnp.float32)
        for j in range(it + 1, 3 * HALO - 1 - it):
            c = state[j]
            s, k = factors[j]
            sc = s * c
            total = upwind(
                sc,
                s,
                jnp.where(low_x, c, pltpu.roll(c, 1, 0)),
                jnp.where(high_x, c, pltpu.roll(c, pitch - 1, 0)),
            )
            total = total + upwind(
                sc,
                s,
                jnp.where(low_y, c, pltpu.roll(c, 1, 1)),
                jnp.where(high_y, c, pltpu.roll(c, 2 * HALF - 1, 1)),
            )
            before, after = state[j - 1], state[j + 1]
            if j == HALO:
                before = jnp.where(low_z, c, before)
            if j == 2 * HALO - 1:
                after = jnp.where(high_z, c, after)
            total = total + upwind(sc, s, before, after)
            new[j] = stepped(c, k, total)
            if HALO <= j < 2 * HALO:
                change = change + (new[j] - c) * (new[j] - c)
        state = new
        change = jnp.where(mine, change, 0.0)
        part = acc_ref[it]
        for t in range(0, pitch, TILE):
            part = part + change[t : t + TILE]
        sums.append(jnp.sum(part, axis=0, keepdims=True))
    for i in range(HALO):
        out_ref[i * pitch : (i + 1) * pitch] = state[HALO + i]
    sums.append(jnp.zeros((TILE - ITERS, 2 * HALF), jnp.float32))
    sum_ref[...] = jnp.concatenate(sums, axis=0)


def merge_kernel(sizes, main_ref, ends_ref, edge_ref, out_ref):
    planes, rows, lanes = sizes
    pitch = edge_ref.shape[0] // HALO
    lane = lax.broadcasted_iota(jnp.int32, (rows, lanes), 1)
    for x in range(planes):
        lines = edge_ref[pl.ds(x + HALO, HALO, stride=pitch)]
        lines = jnp.concatenate(
            [lines, jnp.zeros((lanes - HALO, 2 * HALF), jnp.float32)], axis=0
        )
        turned = lines.T
        near = turned[TILE : TILE + rows]
        far = pltpu.roll(turned[HALF + TILE : HALF + TILE + rows], lanes - HALO, 1)
        if x < HALO:
            main = ends_ref[x]
        elif x >= planes - HALO:
            main = ends_ref[x - planes + 2 * HALO]
        else:
            main = main_ref[x]
        value = jnp.where(lane < HALO, near, main)
        out_ref[x] = jnp.where(lane >= lanes - HALO, far, value)


def vmem(n):
    return [pl.BlockSpec(memory_space=pltpu.VMEM)] * n


def grant(mib):
    return pltpu.CompilerParams(vmem_limit_bytes=mib * 2**20)


def cost(us, nbytes):
    return pl.CostEstimate(flops=int(us * 3.5e6), bytes_accessed=nbytes, transcendentals=0)


def call(kernel, sizes, inputs, outputs, scratch, mib, us):
    return pl.pallas_call(
        functools.partial(kernel, sizes),
        out_shape=tuple(jax.ShapeDtypeStruct(o, jnp.float32) for o in outputs),
        in_specs=vmem(len(inputs)),
        out_specs=tuple(vmem(len(outputs))),
        scratch_shapes=[pltpu.VMEM(t, jnp.float32) for t in scratch],
        compiler_params=grant(mib),
        cost_estimate=cost(us, 10**6),
    )(*inputs)


def local(phi_start):
    sizes = phi_start.shape
    planes, rows, lanes = sizes
    wide = planes + 2 * HALO
    tall = rows + TILE
    pitch = -(-wide // TILE) * TILE

    def mixed(first, second):
        low, high = low_high(first, second, "gy")
        sub = lax.broadcasted_iota(jnp.int32, first.shape, 1)
        return jnp.where(sub < TILE // 2, high, low)

    paired = lax.axis_size("gy") == 2
    kinds = 2 if paired else 1
    if paired:
        (mine,) = call(
            pair_tiles_kernel,
            sizes,
            (phi_start,),
            ((2 * planes * TILE, lanes),),
            (),
            2,
            0.5,
        )
        theirs, _ = exchange(mine, mine, 1)
        mix = theirs[: planes * TILE].reshape(planes, TILE, lanes)
        front_inputs, line_inputs = (phi_start, mix, mine, theirs), (mine, theirs)
    else:
        ys = call(
            tiles_kernel, sizes, (phi_start,), ((planes, TILE, lanes),) * 2, (), 2, 0.2
        )
        mix = mixed(*exchange(ys[0], ys[1], 1))
        front_inputs = line_inputs = (phi_start, mix)

    def with_kinds(kernel):
        return lambda sizes, *refs: kernel(sizes, paired, *refs)

    line, front = (kinds * HALO * TILE, 2 * HALF), (HALO, tall, lanes)
    la, lb, xa, xb = call(
        with_kinds(fronts_kernel),
        sizes,
        front_inputs,
        (line, line, front, front),
        (),
        2,
        0.2,
    )
    la, lb = exchange(la, lb, 0, paired)
    xa, xb = exchange(xa, xb, 0)

    edge_lines = (TILE * pitch, 2 * HALF)
    lines = call(
        with_kinds(lines_kernel), sizes, line_inputs, (edge_lines,) * kinds, (), 2, 0.5
    )
    packed = ((HALO + 1) // 2 * pitch, 2 * HALF)
    strip, sa, sb = call(
        with_kinds(ends_kernel),
        sizes,
        (*lines, la, lb),
        ((3 * HALO * pitch, 2 * HALF), packed, packed),
        (edge_lines,) * kinds,
        4,
        0.2,
    )
    za, zb = exchange(sa, sb, 2, paired)

    block = (planes, tall, lanes)
    e1, e2, inner, s, k, acc = call(
        pre_kernel,
        sizes,
        (phi_start, mix),
        (block, block, sizes, block, block, (ITERS, TILE, lanes)),
        (block,),
        8,
        1.5,
    )
    tips, acc = call(
        post_kernel,
        sizes,
        (phi_start, mix, xa, xb, e1, e2, s, k, acc),
        ((2 * HALO, rows, lanes), (ITERS, TILE, lanes)),
        ((4 * HALO, tall, lanes),) * 2,
        8,
        0.6,
    )

    edge, sums = call(
        edge_kernel,
        sizes,
        (strip, za, zb, acc),
        ((HALO * pitch, 2 * HALF), (TILE, 2 * HALF)),
        (),
        4,
        0.5,
    )

    (phi_final,) = call(merge_kernel, sizes, (inner, tips, edge), (sizes,), (), 4, 1.5)

    totals = jnp.sum(sum_over_devices(sums)[:ITERS], axis=1)
    cells = planes * rows * lanes
    for axis in AXES:
        cells = cells * lax.axis_size(axis)
    residuals = jnp.sqrt(totals / jnp.float32(cells)) / pseudo_step
    return (phi_final, residuals)


def solution(mesh):
    return jax.shard_map(
        local,
        mesh=mesh,
        in_specs=(P("gx", "gy", "gz"),),
        out_specs=(P("gx", "gy", "gz"), P()),
        check_vma=False,
    )
```

```python
import functools

import jax
import jax.numpy as jnp
from jax import lax
from jax.experimental import pallas as pl
from jax.experimental.pallas import tpu as pltpu
from jax.sharding import PartitionSpec as P


ITERS = 3
HALO = ITERS
AXES = ("gx", "gy", "gz")
TILE = 8
HALF = 64

pseudo_step = 0.45


def pair_swap(value, partner):
    sizes = [lax.axis_size(a) for a in AXES]

    def flat(place):
        return (place[0] * sizes[1] + place[1]) * sizes[2] + place[2]

    pairs = []
    for i in range(sizes[0]):
        for j in range(sizes[1]):
            for k in range(sizes[2]):
                pairs.append((flat((i, j, k)), flat(partner((i, j, k)))))
    return lax.ppermute(value, AXES, pairs)


def neighbour(dim, colour, cross):
    sizes = [lax.axis_size(a) for a in AXES]

    def partner(place):
        place = list(place)
        here = place[dim]
        there = here ^ 1 if colour == 0 else ((here - 1) ^ 1) + 1
        if 0 <= there < sizes[dim]:
            place[dim] = there
            if cross:
                place[1] ^= 1
        elif dim != 1 and sizes[1] % 2 == 0:
            place[1] ^= 1
        elif colour == 1 and sizes[dim] % 2 == 0:
            place[dim] = sizes[dim] - 1 - here
        return tuple(place)

    return partner


def exchange(value_even, value_odd, dim, cross=False):
    first = pair_swap(value_even, neighbour(dim, 0, cross))
    if lax.axis_size(AXES[dim]) == 2:
        return first, first
    return first, pair_swap(value_odd, neighbour(dim, 1, cross))


def sum_over_devices(value):
    sizes = [lax.axis_size(a) for a in AXES]
    if any(n & (n - 1) for n in sizes):
        return lax.psum(value, AXES)
    rounds = []
    for dim in (1, 0, 2):
        bit = 1
        while bit < sizes[dim]:
            rounds.append((dim, bit))
            bit *= 2
    crossed = False
    for dim, bit in rounds:

        def partner(place, dim=dim, bit=bit, flip=crossed):
            place = list(place)
            place[dim] ^= bit
            if flip:
                place[1] ^= 1
            return tuple(place)

        value = value + pair_swap(value, partner)
        crossed = crossed or (dim, bit) == (1, 1)
    return value


def at_ends(axis):
    place = lax.axis_index(axis)
    return place == 0, place == lax.axis_size(axis) - 1


def odd(axis):
    return lax.rem(lax.axis_index(axis), 2) == 1


def low_high(first, second, axis):
    is_odd = odd(axis)
    return jnp.where(is_odd, first, second), jnp.where(is_odd, second, first)


def sign_factors(field):
    sgn = field * lax.rsqrt(field * field + 1.0)
    return jnp.where(field > 0.0, 1.0, -1.0), pseudo_step * sgn


def upwind(sc, s, prev, nxt):
    term = jnp.maximum(sc - jnp.minimum(s * prev, s * nxt), 0.0)
    return term * term


def stepped(c, k, total):
    root = total * lax.rsqrt(jnp.maximum(total, 1e-30))
    return c - k * (root - 1.0)


def tiles_kernel(sizes, b_ref, *outs):
    rows = sizes[1]
    y_odd = odd("gy")
    for n, ref in enumerate(outs):
        low = y_odd if n == 0 else ~y_odd
        start = pl.multiple_of(jnp.where(low, 0, rows - TILE), TILE)
        ref[...] = b_ref[:, pl.ds(start, TILE)]


def plane_step(c, s, k, before, after, marks):
    sub, y_first, y_last, rows = marks
    tall, lanes = c.shape
    edge = c[rows:tall]
    edge = jnp.where((sub == TILE - 1) & y_first, c[0:1], edge)
    edge = jnp.where((sub == 0) & y_last, c[rows - 1 : rows], edge)
    around = jnp.concatenate([c[0:rows], edge], axis=0)
    sc = s * c
    total = upwind(sc, s, before, after)
    total = total + upwind(sc, s, pltpu.roll(around, 1, 0), pltpu.roll(around, tall - 1, 0))
    total = total + upwind(sc, s, pltpu.roll(c, 1, 1), pltpu.roll(c, lanes - 1, 1))
    new = stepped(c, k, total)
    change = new[0:rows] - c[0:rows]
    change = change * change
    part = change[0:TILE]
    for t in range(TILE, rows, TILE):
        part = part + change[t : t + TILE]
    return new, part


def plane_marks(sizes):
    _, rows, lanes = sizes
    y_first, y_last = at_ends("gy")
    return lax.broadcasted_iota(jnp.int32, (TILE, lanes), 0), y_first, y_last, rows


def turned_lines(own, mix, lanes):
    turned = jnp.concatenate([mix, own, mix], axis=0).T
    return jnp.concatenate([turned[0:TILE], turned[lanes - TILE : lanes]], axis=1)


def middle(lines_ref, i, pitch, near):
    low = lines_ref[i * pitch : (i + 1) * pitch]
    shift = TILE - HALO
    return jnp.where(near, low, lines_ref[(i + shift) * pitch : (i + shift + 1) * pitch])


def pair_tiles_kernel(sizes, b_ref, out_ref):
    planes, rows, lanes = sizes
    start = pl.multiple_of(jnp.where(odd("gy"), 0, rows - TILE), TILE)
    for p in range(planes):
        plane = b_ref[p]
        out_ref[p * TILE : (p + 1) * TILE] = b_ref[p, pl.ds(start, TILE)]
        out_ref[(planes + p) * TILE : (planes + p + 1) * TILE] = turned_lines(
            plane, plane[0:TILE], lanes
        )


def pair_lines(sizes, mine_ref, theirs_ref):
    planes, rows, _ = sizes
    lane = lax.rem(lax.broadcasted_iota(jnp.int32, (TILE, 2 * HALF), 1), HALF)
    inside = (lane >= TILE) & (lane < TILE + rows)
    y_odd = odd("gy")
    up, down = rows, 2 * HALF - rows

    def lines(p):
        here = slice((planes + p) * TILE, (planes + p + 1) * TILE)
        mine, theirs = mine_ref[here], theirs_ref[here]
        beside_mine = pltpu.roll(theirs, jnp.where(y_odd, down, up), 1)
        beside_theirs = pltpu.roll(mine, jnp.where(y_odd, up, down), 1)
        return jnp.where(inside, mine, beside_mine), jnp.where(inside, theirs, beside_theirs)

    return lines


def own_lines(sizes, b_ref, mix_ref):
    return lambda p: (turned_lines(b_ref[p], mix_ref[p], sizes[2]),)


def fronts_kernel(sizes, paired, b_ref, mix_ref, *refs):
    planes, rows, _ = sizes
    la_ref, lb_ref, xa_ref, xb_ref = refs[-4:]
    lines = pair_lines(sizes, *refs[:2]) if paired else own_lines(sizes, b_ref, mix_ref)
    x_odd = odd("gx")
    for i in range(HALO):
        for n, (low, high) in enumerate(zip(lines(i), lines(planes - HALO + i))):
            here = pl.ds((n * HALO + i) * TILE, TILE)
            la_ref[here] = jnp.where(x_odd, low, high)
            lb_ref[here] = jnp.where(x_odd, high, low)
    sub = lax.broadcasted_iota(jnp.int32, mix_ref.shape[1:], 0)
    for ref, is_low in ((xa_ref, x_odd), (xb_ref, ~x_odd)):
        start = jnp.where(is_low, 0, planes - HALO)
        for i in range(HALO):
            ref[i * rows : (i + 1) * rows] = b_ref[start + i]
        nearest = mix_ref[jnp.where(is_low, 0, planes - 1)]
        second = mix_ref[jnp.where(is_low, 1, planes - 2)]
        nearest = jnp.where(sub == 3, second[0:1], nearest)
        ref[HALO * rows :] = jnp.where(sub == 4, second[TILE - 1 : TILE], nearest)


def lines_kernel(sizes, paired, first_ref, second_ref, *outs):
    planes = sizes[0]
    pitch = outs[0].shape[0] // TILE
    lines = (pair_lines if paired else own_lines)(sizes, first_ref, second_ref)
    for p in range(planes):
        for ref, value in zip(outs, lines(p)):
            ref[pl.ds(p + HALO, TILE, stride=pitch)] = value


def pre_kernel(sizes, b_ref, mix_ref, e1_ref, e2_ref, out_ref, s_ref, k_ref, acc_ref, e0):
    planes, rows, lanes = sizes
    marks = plane_marks(sizes)
    lane = lax.broadcasted_iota(jnp.int32, (TILE, lanes), 1)

    for p in range(planes):
        full = jnp.concatenate([b_ref[p], mix_ref[p]], axis=0)
        e0[p] = full
        s_ref[p], k_ref[p] = sign_factors(full)

    inner = (lane >= HALO) & (lane < lanes - HALO)
    bufs = (e0, e1_ref, e2_ref)
    for it in range(ITERS):

        def body(p, acc, it=it):
            src = bufs[it]
            new, part = plane_step(src[p], s_ref[p], k_ref[p], src[p - 1], src[p + 1], marks)
            if it == ITERS - 1:
                out_ref[p] = new[0:rows]
            else:
                bufs[it + 1][p] = new
            return acc + part

        acc = jnp.zeros((TILE, lanes), jnp.float32)
        acc = lax.fori_loop(it + 1, planes - 1 - it, body, acc, unroll=(7, 6, 5)[it])
        acc_ref[it] = jnp.where(inner, acc, 0.0)


def ends_kernel(sizes, paired, *refs):
    planes = sizes[0]
    kinds = 2 if paired else 1
    la_ref, lb_ref, strip_ref, sa_ref, sb_ref = refs[kinds : kinds + 5]
    sets = refs[kinds + 5 :]
    pitch = refs[0].shape[0] // TILE
    near = lax.broadcasted_iota(jnp.int32, (pitch, 2 * HALF), 1) < HALF
    low, high = low_high(la_ref[...], lb_ref[...], "gx")
    for n in range(kinds):
        lines = sets[n]
        lines[...] = refs[n][...]
        for i in range(HALO):
            k = (kinds - 1 - n) * HALO + i
            here = slice(k * TILE, (k + 1) * TILE)
            lines[pl.ds(i, TILE, stride=pitch)] = low[here]
            lines[pl.ds(i + HALO + planes, TILE, stride=pitch)] = high[here]
    lines, given = sets[0], sets[kinds - 1]
    shift = TILE - 2 * HALO
    for j in range(3 * HALO):
        if j < HALO:
            value = lines[(j + shift) * pitch : (j + shift + 1) * pitch]
        elif j >= 2 * HALO:
            value = lines[(j - HALO) * pitch : (j - HALO + 1) * pitch]
        else:
            value = middle(lines, j - HALO, pitch, near)
        strip_ref[j * pitch : (j + 1) * pitch] = value
    layers = [middle(given, i, pitch, near) for i in range(HALO)]
    swung = [pltpu.roll(v, HALF, 1) for v in layers]
    z_odd = odd("gz")
    for i in range(0, HALO, 2):
        if i + 1 < HALO:
            to_low = jnp.where(near, layers[i], swung[i + 1])
            to_high = jnp.where(near, swung[i], layers[i + 1])
        else:
            to_low, to_high = layers[i], swung[i]
        here = slice(i // 2 * pitch, (i // 2 + 1) * pitch)
        sa_ref[here] = jnp.where(z_odd, to_low, to_high)
        sb_ref[here] = jnp.where(z_odd, to_high, to_low)


def post_kernel(
    sizes,
    b_ref,
    mix_ref,
    xa_ref,
    xb_ref,
    e1_ref,
    e2_ref,
    s_ref,
    k_ref,
    pre_acc_ref,
    out_ref,
    acc_ref,
    f1,
    f2,
):
    planes, rows, lanes = sizes
    x_first, x_last = at_ends("gx")
    marks = plane_marks(sizes)
    lane = lax.broadcasted_iota(jnp.int32, (TILE, lanes), 1)
    inner = (lane >= HALO) & (lane < lanes - HALO)
    sub = lax.broadcasted_iota(jnp.int32, mix_ref.shape[1:], 0)
    factors = {}

    def start(p):
        if 0 <= p < planes:
            return jnp.concatenate([b_ref[p], mix_ref[p]], axis=0)
        i = p + HALO if p < 0 else p - planes
        side = 0 if p < 0 else 1
        low_rows = HALO * rows
        own = low_high(xa_ref[i * rows : (i + 1) * rows], xb_ref[i * rows : (i + 1) * rows], "gx")
        tile = low_high(xa_ref[low_rows : low_rows + TILE], xb_ref[low_rows : low_rows + TILE], "gx")
        tile = tile[side]
        if i == 1:
            tile = jnp.where(sub < TILE // 2, tile[3:4], tile[4:5])
        return jnp.concatenate([own[side], tile], axis=0)

    def factor(p):
        if 0 <= p < planes:
            return s_ref[p], k_ref[p]
        if p not in factors:
            factors[p] = sign_factors(start(p))
        return factors[p]

    def get(it, p):
        if it == 0:
            return start(p)
        if it <= p < planes - it:
            return (e1_ref, e2_ref)[it - 1][p]
        return (f1, f2)[it - 1][p + HALO if p < planes // 2 else p - planes + 3 * HALO]

    for it in range(ITERS):
        acc = jnp.zeros((TILE, lanes), jnp.float32)
        lows = range(it + 1 - HALO, it + 1)
        for p in (*lows, *(planes - 1 - p for p in lows)):
            c = get(it, p)
            before, after = get(it, p - 1), get(it, p + 1)
            if p == 0:
                before = jnp.where(x_first, c, before)
            if p == planes - 1:
                after = jnp.where(x_last, c, after)
            s, k = factor(p)
            new, part = plane_step(c, s, k, before, after, marks)
            if it == ITERS - 1:
                out_ref[p if p < HALO else p - planes + 2 * HALO] = new[0:rows]
            else:
                (f1, f2)[it][p + HALO if p < planes // 2 else p - planes + 3 * HALO] = new
            if 0 <= p < planes:
                acc = acc + part
        acc_ref[it] = pre_acc_ref[it] + jnp.where(inner, acc, 0.0)


def edge_kernel(sizes, strip_ref, za_ref, zb_ref, acc_ref, out_ref, sum_ref):
    planes, rows, _ = sizes
    pitch = strip_ref.shape[0] // (3 * HALO)
    x_first, x_last = at_ends("gx")
    y_first, y_last = at_ends("gy")
    z_first, z_last = at_ends("gz")
    shape = (pitch, 2 * HALF)
    line = lax.broadcasted_iota(jnp.int32, shape, 0)
    lane = lax.broadcasted_iota(jnp.int32, shape, 1)
    near = lane < HALF
    y = jnp.where(near, lane, lane - HALF) - TILE
    x = line - HALO
    low_x = (x == 0) & x_first
    high_x = (x == planes - 1) & x_last
    low_y = (y == 0) & y_first
    high_y = (y == rows - 1) & y_last
    low_z = near & z_first
    high_z = (lane >= HALF) & z_last
    mine = (x >= 0) & (x < planes) & (y >= 0) & (y < rows)

    state = []
    packs = [
        low_high(za_ref[n : n + pitch], zb_ref[n : n + pitch], "gz")
        for n in range(0, za_ref.shape[0], pitch)
    ]
    for j in range(3 * HALO):
        own = strip_ref[j * pitch : (j + 1) * pitch]
        if j < HALO:
            got = packs[j // 2][0]
            got = got if j % 2 == 0 else pltpu.roll(got, HALF, 1)
            own = jnp.where(near, got, own)
        elif j >= 2 * HALO:
            i = j - 2 * HALO
            got = packs[i // 2][1]
            got = pltpu.roll(got, HALF, 1) if i % 2 == 0 else got
            own = jnp.where(near, own, got)
        state.append(own)
    factors = [sign_factors(v) for v in state]

    sums = []
    for it in range(ITERS):
        new = list(state)
        change = jnp.zeros(shape, jnp.float32)
        for j in range(it + 1, 3 * HALO - 1 - it):
            c = state[j]
            s, k = factors[j]
            sc = s * c
            total = upwind(
                sc,
                s,
                jnp.where(low_x, c, pltpu.roll(c, 1, 0)),
                jnp.where(high_x, c, pltpu.roll(c, pitch - 1, 0)),
            )
            total = total + upwind(
                sc,
                s,
                jnp.where(low_y, c, pltpu.roll(c, 1, 1)),
                jnp.where(high_y, c, pltpu.roll(c, 2 * HALF - 1, 1)),
            )
            before, after = state[j - 1], state[j + 1]
            if j == HALO:
                before = jnp.where(low_z, c, before)
            if j == 2 * HALO - 1:
                after = jnp.where(high_z, c, after)
            total = total + upwind(sc, s, before, after)
            new[j] = stepped(c, k, total)
            if HALO <= j < 2 * HALO:
                change = change + (new[j] - c) * (new[j] - c)
        state = new
        change = jnp.where(mine, change, 0.0)
        part = acc_ref[it]
        for t in range(0, pitch, TILE):
            part = part + change[t : t + TILE]
        sums.append(jnp.sum(part, axis=0, keepdims=True))
    for i in range(HALO):
        out_ref[i * pitch : (i + 1) * pitch] = state[HALO + i]
    sums.append(jnp.zeros((TILE - ITERS, 2 * HALF), jnp.float32))
    sum_ref[...] = jnp.concatenate(sums, axis=0)


def merge_kernel(sizes, main_ref, ends_ref, edge_ref, out_ref):
    planes, rows, lanes = sizes
    pitch = edge_ref.shape[0] // HALO
    lane = lax.broadcasted_iota(jnp.int32, (rows, lanes), 1)
    for x in range(planes):
        lines = edge_ref[pl.ds(x + HALO, HALO, stride=pitch)]
        lines = jnp.concatenate(
            [lines, jnp.zeros((lanes - HALO, 2 * HALF), jnp.float32)], axis=0
        )
        turned = lines.T
        near = turned[TILE : TILE + rows]
        far = pltpu.roll(turned[HALF + TILE : HALF + TILE + rows], lanes - HALO, 1)
        if x < HALO:
            main = ends_ref[x]
        elif x >= planes - HALO:
            main = ends_ref[x - planes + 2 * HALO]
        else:
            main = main_ref[x]
        value = jnp.where(lane < HALO, near, main)
        out_ref[x] = jnp.where(lane >= lanes - HALO, far, value)


def vmem(n):
    return [pl.BlockSpec(memory_space=pltpu.VMEM)] * n


def grant(mib):
    return pltpu.CompilerParams(vmem_limit_bytes=mib * 2**20)


def cost(us, nbytes):
    return pl.CostEstimate(flops=int(us * 3.5e6), bytes_accessed=nbytes, transcendentals=0)


def call(kernel, sizes, inputs, outputs, scratch, mib, us):
    return pl.pallas_call(
        functools.partial(kernel, sizes),
        out_shape=tuple(jax.ShapeDtypeStruct(o, jnp.float32) for o in outputs),
        in_specs=vmem(len(inputs)),
        out_specs=tuple(vmem(len(outputs))),
        scratch_shapes=[pltpu.VMEM(t, jnp.float32) for t in scratch],
        compiler_params=grant(mib),
        cost_estimate=cost(us, 10**6),
    )(*inputs)


def local(phi_start):
    sizes = phi_start.shape
    planes, rows, lanes = sizes
    wide = planes + 2 * HALO
    tall = rows + TILE
    pitch = -(-wide // TILE) * TILE

    def mixed(first, second):
        low, high = low_high(first, second, "gy")
        sub = lax.broadcasted_iota(jnp.int32, first.shape, 1)
        return jnp.where(sub < TILE // 2, high, low)

    paired = lax.axis_size("gy") == 2
    kinds = 2 if paired else 1
    if paired:
        (mine,) = call(
            pair_tiles_kernel,
            sizes,
            (phi_start,),
            ((2 * planes * TILE, lanes),),
            (),
            2,
            0.5,
        )
        theirs, _ = exchange(mine, mine, 1)
        mix = theirs[: planes * TILE].reshape(planes, TILE, lanes)
        front_inputs, line_inputs = (phi_start, mix, mine, theirs), (mine, theirs)
    else:
        ys = call(
            tiles_kernel, sizes, (phi_start,), ((planes, TILE, lanes),) * 2, (), 2, 0.2
        )
        mix = mixed(*exchange(ys[0], ys[1], 1))
        front_inputs = line_inputs = (phi_start, mix)

    def with_kinds(kernel):
        return lambda sizes, *refs: kernel(sizes, paired, *refs)

    line, front = (kinds * HALO * TILE, 2 * HALF), (HALO * rows + TILE, lanes)
    la, lb, xa, xb = call(
        with_kinds(fronts_kernel),
        sizes,
        front_inputs,
        (line, line, front, front),
        (),
        2,
        0.2,
    )
    la, lb = exchange(la, lb, 0, paired)
    xa, xb = exchange(xa, xb, 0)

    edge_lines = (TILE * pitch, 2 * HALF)
    lines = call(
        with_kinds(lines_kernel), sizes, line_inputs, (edge_lines,) * kinds, (), 2, 0.5
    )
    packed = ((HALO + 1) // 2 * pitch, 2 * HALF)
    strip, sa, sb = call(
        with_kinds(ends_kernel),
        sizes,
        (*lines, la, lb),
        ((3 * HALO * pitch, 2 * HALF), packed, packed),
        (edge_lines,) * kinds,
        4,
        0.2,
    )
    za, zb = exchange(sa, sb, 2, paired)

    block = (planes, tall, lanes)
    e1, e2, inner, s, k, acc = call(
        pre_kernel,
        sizes,
        (phi_start, mix),
        (block, block, sizes, block, block, (ITERS, TILE, lanes)),
        (block,),
        8,
        1.5,
    )
    tips, acc = call(
        post_kernel,
        sizes,
        (phi_start, mix, xa, xb, e1, e2, s, k, acc),
        ((2 * HALO, rows, lanes), (ITERS, TILE, lanes)),
        ((4 * HALO, tall, lanes),) * 2,
        8,
        0.6,
    )

    edge, sums = call(
        edge_kernel,
        sizes,
        (strip, za, zb, acc),
        ((HALO * pitch, 2 * HALF), (TILE, 2 * HALF)),
        (),
        4,
        0.5,
    )

    (phi_final,) = call(merge_kernel, sizes, (inner, tips, edge), (sizes,), (), 4, 1.5)

    totals = jnp.sum(sum_over_devices(sums)[:ITERS], axis=1)
    cells = planes * rows * lanes
    for axis in AXES:
        cells = cells * lax.axis_size(axis)
    residuals = jnp.sqrt(totals / jnp.float32(cells)) / pseudo_step
    return (phi_final, residuals)


def solution(mesh):
    return jax.shard_map(
        local,
        mesh=mesh,
        in_specs=(P("gx", "gy", "gz"),),
        out_specs=(P("gx", "gy", "gz"), P()),
        check_vma=False,
    )
```

```python
import functools

import jax
import jax.numpy as jnp
from jax import lax
from jax.experimental import pallas as pl
from jax.experimental.pallas import tpu as pltpu
from jax.sharding import PartitionSpec as P


ITERS = 3
HALO = ITERS
AXES = ("gx", "gy", "gz")
TILE = 8
HALF = 64
GROUP = 32
DIRECT = 64

pseudo_step = 0.45


def pair_swap(value, partner):
    sizes = [lax.axis_size(a) for a in AXES]

    def flat(place):
        return (place[0] * sizes[1] + place[1]) * sizes[2] + place[2]

    pairs = []
    for i in range(sizes[0]):
        for j in range(sizes[1]):
            for k in range(sizes[2]):
                pairs.append((flat((i, j, k)), flat(partner((i, j, k)))))
    return lax.ppermute(value, AXES, pairs)


def neighbour(dim, colour, cross):
    sizes = [lax.axis_size(a) for a in AXES]

    def partner(place):
        place = list(place)
        here = place[dim]
        there = here ^ 1 if colour == 0 else ((here - 1) ^ 1) + 1
        if 0 <= there < sizes[dim]:
            place[dim] = there
            if cross:
                place[1] ^= 1
        elif dim != 1 and sizes[1] % 2 == 0:
            place[1] ^= 1
        elif colour == 1 and sizes[dim] % 2 == 0:
            place[dim] = sizes[dim] - 1 - here
        return tuple(place)

    return partner


def exchange(value_even, value_odd, dim, cross=False):
    first = pair_swap(value_even, neighbour(dim, 0, cross))
    if lax.axis_size(AXES[dim]) == 2:
        return first, first
    return first, pair_swap(value_odd, neighbour(dim, 1, cross))


def sum_over_devices(value):
    sizes = [lax.axis_size(a) for a in AXES]
    if value.shape[0] > 1:
        return jnp.sum(lax.all_to_all(value, AXES, 0, 0), axis=0, keepdims=True)
    if any(n & (n - 1) for n in sizes):
        return lax.psum(value, AXES)
    rounds = []
    for dim in (1, 0, 2):
        bit = 1
        while bit < sizes[dim]:
            rounds.append((dim, bit))
            bit *= 2
    crossed = False
    for dim, bit in rounds:

        def partner(place, dim=dim, bit=bit, flip=crossed):
            place = list(place)
            place[dim] ^= bit
            if flip:
                place[1] ^= 1
            return tuple(place)

        value = value + pair_swap(value, partner)
        crossed = crossed or (dim, bit) == (1, 1)
    return value


def at_ends(axis):
    place = lax.axis_index(axis)
    return place == 0, place == lax.axis_size(axis) - 1


def odd(axis):
    return lax.rem(lax.axis_index(axis), 2) == 1


def low_high(first, second, axis):
    is_odd = odd(axis)
    return jnp.where(is_odd, first, second), jnp.where(is_odd, second, first)


def sign_factors(field):
    sgn = field * lax.rsqrt(field * field + 1.0)
    return jnp.where(field > 0.0, 1.0, -1.0), pseudo_step * sgn


def upwind(sc, s, prev, nxt):
    term = jnp.maximum(sc - jnp.minimum(s * prev, s * nxt), 0.0)
    return term * term


def stepped(c, k, total):
    root = total * lax.rsqrt(jnp.maximum(total, 1e-30))
    return c - k * (root - 1.0)


def tiles_kernel(sizes, b_ref, *outs):
    rows = sizes[1]
    y_odd = odd("gy")
    for n, ref in enumerate(outs):
        low = y_odd if n == 0 else ~y_odd
        start = pl.multiple_of(jnp.where(low, 0, rows - TILE), TILE)
        ref[...] = b_ref[:, pl.ds(start, TILE)]


def plane_step(c, s, k, before, after, marks):
    sub, y_first, y_last, rows = marks
    tall, lanes = c.shape
    edge = c[rows:tall]
    edge = jnp.where((sub == TILE - 1) & y_first, c[0:1], edge)
    edge = jnp.where((sub == 0) & y_last, c[rows - 1 : rows], edge)
    around = jnp.concatenate([c[0:rows], edge], axis=0)
    sc = s * c
    total = upwind(sc, s, before, after)
    total = total + upwind(sc, s, pltpu.roll(around, 1, 0), pltpu.roll(around, tall - 1, 0))
    total = total + upwind(sc, s, pltpu.roll(c, 1, 1), pltpu.roll(c, lanes - 1, 1))
    new = stepped(c, k, total)
    change = new[0:rows] - c[0:rows]
    change = change * change
    part = change[0:TILE]
    for t in range(TILE, rows, TILE):
        part = part + change[t : t + TILE]
    return new, part


def plane_marks(sizes):
    _, rows, lanes = sizes
    y_first, y_last = at_ends("gy")
    return lax.broadcasted_iota(jnp.int32, (TILE, lanes), 0), y_first, y_last, rows


def turned_lines(own, mix, lanes):
    turned = jnp.concatenate([mix, own, mix], axis=0).T
    return jnp.concatenate([turned[0:TILE], turned[lanes - TILE : lanes]], axis=1)


def middle(lines_ref, i, pitch, near):
    low = lines_ref[i * pitch : (i + 1) * pitch]
    shift = TILE - HALO
    return jnp.where(near, low, lines_ref[(i + shift) * pitch : (i + shift + 1) * pitch])


def pair_tiles_kernel(sizes, b_ref, out_ref):
    planes, rows, lanes = sizes
    start = pl.multiple_of(jnp.where(odd("gy"), 0, rows - TILE), TILE)
    for p in range(planes):
        plane = b_ref[p]
        out_ref[p * TILE : (p + 1) * TILE] = b_ref[p, pl.ds(start, TILE)]
        out_ref[(planes + p) * TILE : (planes + p + 1) * TILE] = turned_lines(
            plane, plane[0:TILE], lanes
        )


def pair_lines(sizes, mine_ref, theirs_ref):
    planes, rows, _ = sizes
    lane = lax.rem(lax.broadcasted_iota(jnp.int32, (TILE, 2 * HALF), 1), HALF)
    inside = (lane >= TILE) & (lane < TILE + rows)
    y_odd = odd("gy")
    up, down = rows, 2 * HALF - rows

    def lines(p):
        here = slice((planes + p) * TILE, (planes + p + 1) * TILE)
        mine, theirs = mine_ref[here], theirs_ref[here]
        beside_mine = pltpu.roll(theirs, jnp.where(y_odd, down, up), 1)
        beside_theirs = pltpu.roll(mine, jnp.where(y_odd, up, down), 1)
        return jnp.where(inside, mine, beside_mine), jnp.where(inside, theirs, beside_theirs)

    return lines


def own_lines(sizes, b_ref, mix_ref):
    return lambda p: (turned_lines(b_ref[p], mix_ref[p], sizes[2]),)


def fronts_kernel(sizes, paired, b_ref, mix_ref, *refs):
    planes, rows, _ = sizes
    la_ref, lb_ref, xa_ref, xb_ref = refs[-4:]
    lines = pair_lines(sizes, *refs[:2]) if paired else own_lines(sizes, b_ref, mix_ref)
    x_odd = odd("gx")
    for i in range(HALO):
        for n, (low, high) in enumerate(zip(lines(i), lines(planes - HALO + i))):
            here = pl.ds((n * HALO + i) * TILE, TILE)
            la_ref[here] = jnp.where(x_odd, low, high)
            lb_ref[here] = jnp.where(x_odd, high, low)
    sub = lax.broadcasted_iota(jnp.int32, mix_ref.shape[1:], 0)
    for ref, is_low in ((xa_ref, x_odd), (xb_ref, ~x_odd)):
        start = jnp.where(is_low, 0, planes - HALO)
        for i in range(HALO):
            ref[i * rows : (i + 1) * rows] = b_ref[start + i]
        nearest = mix_ref[jnp.where(is_low, 0, planes - 1)]
        second = mix_ref[jnp.where(is_low, 1, planes - 2)]
        nearest = jnp.where(sub == 3, second[0:1], nearest)
        ref[HALO * rows :] = jnp.where(sub == 4, second[TILE - 1 : TILE], nearest)


def lines_kernel(sizes, paired, first_ref, second_ref, *outs):
    planes = sizes[0]
    pitch = outs[0].shape[0] // TILE
    lines = (pair_lines if paired else own_lines)(sizes, first_ref, second_ref)
    for p in range(planes):
        for ref, value in zip(outs, lines(p)):
            ref[pl.ds(p + HALO, TILE, stride=pitch)] = value


def pre_kernel(sizes, b_ref, mix_ref, e1_ref, e2_ref, out_ref, s_ref, k_ref, acc_ref, e0):
    planes, rows, lanes = sizes
    marks = plane_marks(sizes)
    lane = lax.broadcasted_iota(jnp.int32, (TILE, lanes), 1)

    for p in range(planes):
        full = jnp.concatenate([b_ref[p], mix_ref[p]], axis=0)
        e0[p] = full
        s_ref[p], k_ref[p] = sign_factors(full)

    inner = (lane >= HALO) & (lane < lanes - HALO)
    bufs = (e0, e1_ref, e2_ref)
    for it in range(ITERS):

        def body(p, acc, it=it):
            src = bufs[it]
            new, part = plane_step(src[p], s_ref[p], k_ref[p], src[p - 1], src[p + 1], marks)
            if it == ITERS - 1:
                out_ref[p] = new[0:rows]
            else:
                bufs[it + 1][p] = new
            return acc + part

        acc = jnp.zeros((TILE, lanes), jnp.float32)
        acc = lax.fori_loop(it + 1, planes - 1 - it, body, acc, unroll=(7, 6, 5)[it])
        acc_ref[it] = jnp.where(inner, acc, 0.0)


def ends_kernel(sizes, paired, *refs):
    planes = sizes[0]
    kinds = 2 if paired else 1
    la_ref, lb_ref, strip_ref, sa_ref, sb_ref = refs[kinds : kinds + 5]
    sets = refs[kinds + 5 :]
    pitch = refs[0].shape[0] // TILE
    near = lax.broadcasted_iota(jnp.int32, (pitch, 2 * HALF), 1) < HALF
    low, high = low_high(la_ref[...], lb_ref[...], "gx")
    for n in range(kinds):
        lines = sets[n]
        lines[...] = refs[n][...]
        for i in range(HALO):
            k = (kinds - 1 - n) * HALO + i
            here = slice(k * TILE, (k + 1) * TILE)
            lines[pl.ds(i, TILE, stride=pitch)] = low[here]
            lines[pl.ds(i + HALO + planes, TILE, stride=pitch)] = high[here]
    lines, given = sets[0], sets[kinds - 1]
    shift = TILE - 2 * HALO
    for j in range(3 * HALO):
        if j < HALO:
            value = lines[(j + shift) * pitch : (j + shift + 1) * pitch]
        elif j >= 2 * HALO:
            value = lines[(j - HALO) * pitch : (j - HALO + 1) * pitch]
        else:
            value = middle(lines, j - HALO, pitch, near)
        strip_ref[j * pitch : (j + 1) * pitch] = value
    layers = [middle(given, i, pitch, near) for i in range(HALO)]
    swung = [pltpu.roll(v, HALF, 1) for v in layers]
    z_odd = odd("gz")
    for i in range(0, HALO, 2):
        if i + 1 < HALO:
            to_low = jnp.where(near, layers[i], swung[i + 1])
            to_high = jnp.where(near, swung[i], layers[i + 1])
        else:
            to_low, to_high = layers[i], swung[i]
        here = slice(i // 2 * pitch, (i // 2 + 1) * pitch)
        sa_ref[here] = jnp.where(z_odd, to_low, to_high)
        sb_ref[here] = jnp.where(z_odd, to_high, to_low)


def post_kernel(
    sizes,
    b_ref,
    mix_ref,
    xa_ref,
    xb_ref,
    e1_ref,
    e2_ref,
    s_ref,
    k_ref,
    pre_acc_ref,
    out_ref,
    acc_ref,
    f1,
    f2,
):
    planes, rows, lanes = sizes
    x_first, x_last = at_ends("gx")
    marks = plane_marks(sizes)
    lane = lax.broadcasted_iota(jnp.int32, (TILE, lanes), 1)
    inner = (lane >= HALO) & (lane < lanes - HALO)
    sub = lax.broadcasted_iota(jnp.int32, mix_ref.shape[1:], 0)
    factors = {}

    def start(p):
        if 0 <= p < planes:
            return jnp.concatenate([b_ref[p], mix_ref[p]], axis=0)
        i = p + HALO if p < 0 else p - planes
        side = 0 if p < 0 else 1
        low_rows = HALO * rows
        own = low_high(xa_ref[i * rows : (i + 1) * rows], xb_ref[i * rows : (i + 1) * rows], "gx")
        tile = low_high(xa_ref[low_rows : low_rows + TILE], xb_ref[low_rows : low_rows + TILE], "gx")
        tile = tile[side]
        if i == 1:
            tile = jnp.where(sub < TILE // 2, tile[3:4], tile[4:5])
        return jnp.concatenate([own[side], tile], axis=0)

    def factor(p):
        if 0 <= p < planes:
            return s_ref[p], k_ref[p]
        if p not in factors:
            factors[p] = sign_factors(start(p))
        return factors[p]

    def get(it, p):
        if it == 0:
            return start(p)
        if it <= p < planes - it:
            return (e1_ref, e2_ref)[it - 1][p]
        return (f1, f2)[it - 1][p + HALO if p < planes // 2 else p - planes + 3 * HALO]

    for it in range(ITERS):
        acc = jnp.zeros((TILE, lanes), jnp.float32)
        lows = range(it + 1 - HALO, it + 1)
        for p in (*lows, *(planes - 1 - p for p in lows)):
            c = get(it, p)
            before, after = get(it, p - 1), get(it, p + 1)
            if p == 0:
                before = jnp.where(x_first, c, before)
            if p == planes - 1:
                after = jnp.where(x_last, c, after)
            s, k = factor(p)
            new, part = plane_step(c, s, k, before, after, marks)
            if it == ITERS - 1:
                out_ref[p if p < HALO else p - planes + 2 * HALO] = new[0:rows]
            else:
                (f1, f2)[it][p + HALO if p < planes // 2 else p - planes + 3 * HALO] = new
            if 0 <= p < planes:
                acc = acc + part
        acc_ref[it] = pre_acc_ref[it] + jnp.where(inner, acc, 0.0)


def edge_kernel(sizes, strip_ref, za_ref, zb_ref, acc_ref, out_ref, sum_ref):
    planes, rows, _ = sizes
    pitch = strip_ref.shape[0] // (3 * HALO)
    x_first, x_last = at_ends("gx")
    y_first, y_last = at_ends("gy")
    z_first, z_last = at_ends("gz")
    shape = (pitch, 2 * HALF)
    line = lax.broadcasted_iota(jnp.int32, shape, 0)
    lane = lax.broadcasted_iota(jnp.int32, shape, 1)
    near = lane < HALF
    y = jnp.where(near, lane, lane - HALF) - TILE
    x = line - HALO
    low_x = (x == 0) & x_first
    high_x = (x == planes - 1) & x_last
    low_y = (y == 0) & y_first
    high_y = (y == rows - 1) & y_last
    low_z = near & z_first
    high_z = (lane >= HALF) & z_last
    mine = (x >= 0) & (x < planes) & (y >= 0) & (y < rows)

    state = []
    packs = [
        low_high(za_ref[n : n + pitch], zb_ref[n : n + pitch], "gz")
        for n in range(0, za_ref.shape[0], pitch)
    ]
    for j in range(3 * HALO):
        own = strip_ref[j * pitch : (j + 1) * pitch]
        if j < HALO:
            got = packs[j // 2][0]
            got = got if j % 2 == 0 else pltpu.roll(got, HALF, 1)
            own = jnp.where(near, got, own)
        elif j >= 2 * HALO:
            i = j - 2 * HALO
            got = packs[i // 2][1]
            got = pltpu.roll(got, HALF, 1) if i % 2 == 0 else got
            own = jnp.where(near, own, got)
        state.append(own)
    factors = [sign_factors(v) for v in state]

    sums = []
    for it in range(ITERS):
        new = list(state)
        change = jnp.zeros(shape, jnp.float32)
        for j in range(it + 1, 3 * HALO - 1 - it):
            c = state[j]
            s, k = factors[j]
            sc = s * c
            total = upwind(
                sc,
                s,
                jnp.where(low_x, c, pltpu.roll(c, 1, 0)),
                jnp.where(high_x, c, pltpu.roll(c, pitch - 1, 0)),
            )
            total = total + upwind(
                sc,
                s,
                jnp.where(low_y, c, pltpu.roll(c, 1, 1)),
                jnp.where(high_y, c, pltpu.roll(c, 2 * HALF - 1, 1)),
            )
            before, after = state[j - 1], state[j + 1]
            if j == HALO:
                before = jnp.where(low_z, c, before)
            if j == 2 * HALO - 1:
                after = jnp.where(high_z, c, after)
            total = total + upwind(sc, s, before, after)
            new[j] = stepped(c, k, total)
            if HALO <= j < 2 * HALO:
                change = change + (new[j] - c) * (new[j] - c)
        state = new
        change = jnp.where(mine, change, 0.0)
        part = acc_ref[it]
        for t in range(0, pitch, TILE):
            part = part + change[t : t + TILE]
        sums.append(jnp.sum(part, axis=0, keepdims=True))
    for i in range(HALO):
        out_ref[i * pitch : (i + 1) * pitch] = state[HALO + i]
    groups = lax.broadcasted_iota(jnp.int32, (1, 2 * HALF), 1) // GROUP
    row = jnp.zeros((1, 2 * HALF), jnp.float32)
    for it, part in enumerate(sums):
        width = 2 * HALF
        while width > GROUP:
            width //= 2
            part = part + pltpu.roll(part, width, 1)
        row = jnp.where(groups == it, part, row)
    sum_ref[...] = jnp.broadcast_to(row[None], sum_ref.shape)


def merge_kernel(sizes, main_ref, ends_ref, edge_ref, out_ref):
    planes, rows, lanes = sizes
    pitch = edge_ref.shape[0] // HALO
    lane = lax.broadcasted_iota(jnp.int32, (rows, lanes), 1)
    for x in range(planes):
        lines = edge_ref[pl.ds(x + HALO, HALO, stride=pitch)]
        lines = jnp.concatenate(
            [lines, jnp.zeros((lanes - HALO, 2 * HALF), jnp.float32)], axis=0
        )
        turned = lines.T
        near = turned[TILE : TILE + rows]
        far = pltpu.roll(turned[HALF + TILE : HALF + TILE + rows], lanes - HALO, 1)
        if x < HALO:
            main = ends_ref[x]
        elif x >= planes - HALO:
            main = ends_ref[x - planes + 2 * HALO]
        else:
            main = main_ref[x]
        value = jnp.where(lane < HALO, near, main)
        out_ref[x] = jnp.where(lane >= lanes - HALO, far, value)


def vmem(n):
    return [pl.BlockSpec(memory_space=pltpu.VMEM)] * n


def grant(mib):
    return pltpu.CompilerParams(vmem_limit_bytes=mib * 2**20)


def cost(us, nbytes):
    return pl.CostEstimate(flops=int(us * 3.5e6), bytes_accessed=nbytes, transcendentals=0)


def call(kernel, sizes, inputs, outputs, scratch, mib, us):
    return pl.pallas_call(
        functools.partial(kernel, sizes),
        out_shape=tuple(jax.ShapeDtypeStruct(o, jnp.float32) for o in outputs),
        in_specs=vmem(len(inputs)),
        out_specs=tuple(vmem(len(outputs))),
        scratch_shapes=[pltpu.VMEM(t, jnp.float32) for t in scratch],
        compiler_params=grant(mib),
        cost_estimate=cost(us, 10**6),
    )(*inputs)


def local(phi_start):
    sizes = phi_start.shape
    planes, rows, lanes = sizes
    wide = planes + 2 * HALO
    tall = rows + TILE
    pitch = -(-wide // TILE) * TILE

    def mixed(first, second):
        low, high = low_high(first, second, "gy")
        sub = lax.broadcasted_iota(jnp.int32, first.shape, 1)
        return jnp.where(sub < TILE // 2, high, low)

    paired = lax.axis_size("gy") == 2
    kinds = 2 if paired else 1
    if paired:
        (mine,) = call(
            pair_tiles_kernel,
            sizes,
            (phi_start,),
            ((2 * planes * TILE, lanes),),
            (),
            2,
            0.5,
        )
        theirs, _ = exchange(mine, mine, 1)
        mix = theirs[: planes * TILE].reshape(planes, TILE, lanes)
        front_inputs, line_inputs = (phi_start, mix, mine, theirs), (mine, theirs)
    else:
        ys = call(
            tiles_kernel, sizes, (phi_start,), ((planes, TILE, lanes),) * 2, (), 2, 0.2
        )
        mix = mixed(*exchange(ys[0], ys[1], 1))
        front_inputs = line_inputs = (phi_start, mix)

    def with_kinds(kernel):
        return lambda sizes, *refs: kernel(sizes, paired, *refs)

    line, front = (kinds * HALO * TILE, 2 * HALF), (HALO * rows + TILE, lanes)
    la, lb, xa, xb = call(
        with_kinds(fronts_kernel),
        sizes,
        front_inputs,
        (line, line, front, front),
        (),
        2,
        0.2,
    )
    la, lb = exchange(la, lb, 0, paired)
    xa, xb = exchange(xa, xb, 0)

    edge_lines = (TILE * pitch, 2 * HALF)
    lines = call(
        with_kinds(lines_kernel), sizes, line_inputs, (edge_lines,) * kinds, (), 2, 0.5
    )
    packed = ((HALO + 1) // 2 * pitch, 2 * HALF)
    strip, sa, sb = call(
        with_kinds(ends_kernel),
        sizes,
        (*lines, la, lb),
        ((3 * HALO * pitch, 2 * HALF), packed, packed),
        (edge_lines,) * kinds,
        4,
        0.2,
    )
    za, zb = exchange(sa, sb, 2, paired)

    block = (planes, tall, lanes)
    e1, e2, inner, s, k, acc = call(
        pre_kernel,
        sizes,
        (phi_start, mix),
        (block, block, sizes, block, block, (ITERS, TILE, lanes)),
        (block,),
        8,
        1.5,
    )
    tips, acc = call(
        post_kernel,
        sizes,
        (phi_start, mix, xa, xb, e1, e2, s, k, acc),
        ((2 * HALO, rows, lanes), (ITERS, TILE, lanes)),
        ((4 * HALO, tall, lanes),) * 2,
        8,
        0.6,
    )

    devices = 1
    for axis in AXES:
        devices = devices * lax.axis_size(axis)
    edge, sums = call(
        edge_kernel,
        sizes,
        (strip, za, zb, acc),
        ((HALO * pitch, 2 * HALF), (devices if devices <= DIRECT else 1, 1, 2 * HALF)),
        (),
        4,
        0.5,
    )

    (phi_final,) = call(merge_kernel, sizes, (inner, tips, edge), (sizes,), (), 4, 1.5)

    row = sum_over_devices(sums).reshape(1, 2 * HALF)
    groups = lax.broadcasted_iota(jnp.int32, (ITERS, 2 * HALF), 1) // GROUP
    wanted = lax.broadcasted_iota(jnp.int32, (ITERS, 2 * HALF), 0)
    totals = jnp.sum(jnp.where(groups == wanted, row, 0.0), axis=1)
    cells = planes * rows * lanes * devices
    residuals = jnp.sqrt(totals / jnp.float32(cells)) / pseudo_step
    return (phi_final, residuals)


def solution(mesh):
    return jax.shard_map(
        local,
        mesh=mesh,
        in_specs=(P("gx", "gy", "gz"),),
        out_specs=(P("gx", "gy", "gz"), P()),
        check_vma=False,
    )
```
